128 devices in a mesh: ctx: 32 (over x, z_lo, y), tp: 4 (over z_hi, core).
Axes of the slice: x: 4, y: 4, z: 4 (z_hi: 2, z_lo: 2; z = z_hi * 2 + z_lo), core: 2. Of those that a mesh axis runs over, the one named last changes fastest.
Arguments:
- resid: bfloat16 [65536, 4096], P('ctx', 'tp'), may hold values from -6 to 6
- sel_blocks: int32 [64], P('ctx'), may hold values from 0 to 511, as said below
- norm_gain: float32 [4096], replicated, may hold values from 0.5 to 1.5
- router_weight: float32 [4096], replicated, may hold values from -0.09375 to 0.09375
- w_query: bfloat16 [4096, 4096], P(None, 'tp'), may hold values from -0.25 to 0.25
- w_key: bfloat16 [4096, 512], P(None, 'tp'), may hold values from -4 to 4
- value_projection: bfloat16 [4096, 512], P(None, 'tp'), may hold values from -0.09375 to 0.09375
- w_out: bfloat16 [4096, 4096], P('tp'), may hold values from -0.09375 to 0.09375
Outputs:
- mixed: bfloat16 [8192, 4096], P(('ctx', 'tp'))
The draws below stay inside these ranges and needn't reach their ends.
Inputs may be any that keep to these rules, and one draw needn't show every extreme that they name: `sel_blocks`: entries 2 * c to 2 * c + 1 are 2 different numbers from c * 16 to c * 16 + 15, increasing.
All inputs are finite; a program needn't handle non-finite values.
Results may differ from the reference program's by a relative error of at most 0.0075.
Values may be sent and summed in bfloat16 or wider, within the bound.
A program may use at most 128 MiB of HBM per device.

```python
import math
import jax
import jax.numpy as jnp
from jax import lax

MODEL_WIDTH = 4096
HEAD_WIDTH = 128
KEY_VALUE_HEADS = 4
QUERY_GROUP_SIZE = 8
BLK = 128
NBLK_DEV = 16
HQ = 32
SEL_DEV = 2
TOKENS = 65536
NBLK = 512
SELECTED_ROWS = 8192


def pick_blocks(key):
    devices = NBLK // NBLK_DEV
    scores = jax.random.randint(key, (devices, NBLK_DEV), 0, 1 << 20) * NBLK_DEV + jnp.arange(NBLK_DEV, dtype=jnp.int32)[None, :]
    unused, picked = lax.top_k(scores, SEL_DEV)
    picked = jnp.sort(picked, axis=1)
    return (picked + jnp.arange(devices, dtype=jnp.int32)[:, None] * NBLK_DEV).reshape(devices * SEL_DEV).astype(jnp.int32)


def draw_sel_blocks(key, part):
    return pick_blocks(jax.random.fold_in(key, 3))


def attention_weights(key):
    base_key = jax.random.fold_in(key, 7)
    initial_random_key, middle_random_key = jax.random.split(base_key, 2)
    query_lookup_table = jax.random.normal(initial_random_key, (MODEL_WIDTH, KEY_VALUE_HEADS, QUERY_GROUP_SIZE, HEAD_WIDTH), jnp.float32) / math.sqrt(MODEL_WIDTH)
    key_lookup_table = 3.0 * jax.random.normal(middle_random_key, (MODEL_WIDTH, KEY_VALUE_HEADS, HEAD_WIDTH), jnp.float32) / math.sqrt(MODEL_WIDTH)
    query_lookup_table = jnp.clip(query_lookup_table, -0.25, 0.25).reshape(MODEL_WIDTH, HQ * HEAD_WIDTH)
    key_lookup_table = jnp.clip(key_lookup_table, -4.0, 4.0).reshape(MODEL_WIDTH, KEY_VALUE_HEADS * HEAD_WIDTH)
    return (query_lookup_table, key_lookup_table)


def draw_w_query(key, part):
    return attention_weights(key)[0].astype(jnp.bfloat16)


def draw_w_key(key, part):
    return attention_weights(key)[1].astype(jnp.bfloat16)


def level_of(key, dims, cuts, smallest, top_value):
    def one(dim, blocks):
        draws = jax.random.uniform(jax.random.fold_in(jax.random.fold_in(key, 6), dim), (blocks,), jnp.float32, smallest / len(cuts), top_value / len(cuts))
        return jnp.repeat(jnp.exp(draws), dims[dim] // blocks).reshape((-1,) + (1,) * (len(dims) - dim - 1))

    factor_of = one(*cuts[0])
    for cut in cuts[1:]:
        factor_of = factor_of * one(*cut)
    return factor_of


def noise(stream_key, extent, width, bound, shards=(), held_as=jnp.bfloat16):
    factor_of = level_of(stream_key, extent, shards, -0.22, 0.18) if shards else 1.0
    array = jax.random.normal(stream_key, extent, jnp.float32) * width * factor_of
    return jnp.minimum(jnp.maximum(array, -bound), bound).astype(held_as)


def setup_inputs(seed: int = 0) -> dict:
    key_list = jax.random.split(jax.random.key(seed), 9)
    resid = noise(key_list[0], (TOKENS, MODEL_WIDTH), 1.0, 6.0, ((0, 32), (1, 4)))
    sel_blocks = draw_sel_blocks(jax.random.fold_in(key_list[8], 71), 0)
    norm_gain = jnp.clip(1.0 + 0.1 * jax.random.normal(key_list[2], (MODEL_WIDTH,), jnp.float32), 0.5, 1.5)
    router_weight = noise(key_list[3], (MODEL_WIDTH,), MODEL_WIDTH ** -0.5, 0.09375, (), jnp.float32)
    w_query = draw_w_query(jax.random.fold_in(key_list[8], 71), 0)
    w_key = draw_w_key(jax.random.fold_in(key_list[8], 71), 0)
    value_projection = noise(key_list[6], (MODEL_WIDTH, KEY_VALUE_HEADS * HEAD_WIDTH), MODEL_WIDTH ** -0.5, 0.09375, ((1, 4),))
    w_out = noise(key_list[7], (HQ * HEAD_WIDTH, MODEL_WIDTH), (HQ * HEAD_WIDTH) ** -0.5, 0.09375, ((0, 4),))
    return dict(resid=resid, sel_blocks=sel_blocks, norm_gain=norm_gain, router_weight=router_weight, w_query=w_query, w_key=w_key, value_projection=value_projection, w_out=w_out)


rope_base = 500000.0
norm_eps = 1e-05

def rotate_heads(values_in, positions, head_size):
    rows = values_in.shape[0]
    heads = values_in.shape[1] // head_size
    shaped = values_in.reshape(rows, heads, head_size)
    half_size = head_size // 2
    freqs = jnp.exp(jnp.arange(half_size, dtype=jnp.float32) * (-2.0 * math.log(rope_base) / head_size))
    angles = positions.astype(jnp.float32)[:, None] * freqs[None, :]
    cosine = jnp.cos(angles)[:, None, :]
    sine = jnp.sin(angles)[:, None, :]
    first = shaped[:, :, :half_size]
    second = shaped[:, :, half_size:]
    turned = jnp.concatenate([first * cosine - second * sine, second * cosine + first * sine], axis=2)
    return turned.reshape(rows, heads * head_size).astype(jnp.bfloat16)

def reference(resid, sel_blocks, norm_gain, router_weight, w_query, w_key, value_projection, w_out):
    position = (sel_blocks[:, None] * BLK + jnp.arange(BLK, dtype=jnp.int32)[None, :]).reshape(SELECTED_ROWS).astype(jnp.int32)
    chosen = resid[position]
    chosen_wide = chosen.astype(jnp.float32)
    inv_rms = lax.rsqrt(lax.optimization_barrier(jnp.mean(chosen_wide * chosen_wide, axis=1)) + norm_eps)
    normed = (chosen_wide * inv_rms[:, None] * norm_gain[None, :]).astype(jnp.bfloat16)
    gate = jax.nn.sigmoid(lax.optimization_barrier(jnp.sum(chosen_wide * router_weight[None, :], axis=1)))
    queries = rotate_heads(jnp.dot(normed, w_query, preferred_element_type=jnp.float32), position, HEAD_WIDTH)
    key_matrix = rotate_heads(jnp.dot(normed, w_key, preferred_element_type=jnp.float32), position, HEAD_WIDTH)
    value_matrix = jnp.dot(normed, value_projection, preferred_element_type=jnp.float32).astype(jnp.bfloat16)
    query_heads = queries.reshape(SELECTED_ROWS, HQ, HEAD_WIDTH).transpose(1, 0, 2)
    per_head_keys = key_matrix.reshape(SELECTED_ROWS, KEY_VALUE_HEADS, HEAD_WIDTH).transpose(1, 0, 2)
    per_head_values = value_matrix.reshape(SELECTED_ROWS, KEY_VALUE_HEADS, HEAD_WIDTH).transpose(1, 0, 2)
    allowed = position[None, :] <= position[:, None]
    score_scale = 1.0 / math.sqrt(HEAD_WIDTH)

    def one_head(head):
        query_one = query_heads[head]
        key_one = per_head_keys[head // QUERY_GROUP_SIZE]
        value_one = per_head_values[head // QUERY_GROUP_SIZE]
        scores = jnp.dot(query_one, key_one.T, preferred_element_type=jnp.float32) * score_scale
        scores = jnp.where(allowed, scores, -jnp.inf)
        highest = lax.optimization_barrier(jnp.max(scores, axis=1, keepdims=True))
        expd = jnp.exp(scores - highest)
        weights = expd.astype(jnp.bfloat16)
        mixed_values = jnp.dot(weights, value_one, preferred_element_type=jnp.float32)
        return (mixed_values / lax.optimization_barrier(jnp.sum(expd, axis=1, keepdims=True))).astype(jnp.bfloat16)
    per_head = lax.map(one_head, jnp.arange(HQ, dtype=jnp.int32))
    attended = per_head.transpose(1, 0, 2).reshape(SELECTED_ROWS, HQ * HEAD_WIDTH)
    projected = jnp.dot(attended, w_out, preferred_element_type=jnp.float32)
    return (chosen_wide + gate[:, None] * projected).astype(jnp.bfloat16)
```

```python
import math

import jax
import jax.numpy as jnp
from jax import lax
from jax.experimental import pallas as pl
from jax.experimental.pallas import tpu as pltpu
from jax.sharding import PartitionSpec as P

HEAD = 128
BLK = 128
MESH = pl.DeviceIdType.MESH
BF = jnp.bfloat16
F32 = jnp.float32

rope_base = 500000.0
norm_eps = 1e-05
LOW = -1e30


def dot(a, b):
    return jnp.dot(a, b, preferred_element_type=F32)


def layer_kernel(
    own, cosf, sinf, gain, router, wq_hbm, wk_hbm, wv_hbm, wo_hbm,
    out,
    wq, wkv, wo, part, zsame, zother, rel_p, rel_m,
    qacc, kvacc, ssq, gsum, q, buf_a, buf_b, m_ref, acc, att,
    prem, ploc, d_out, d_in, dl_out, dl_in, zs_out, zr_rel, zr_in,
    ssem, rsem, wsem,
):
    c = lax.axis_index("ctx")
    t = lax.axis_index("tp")
    x, zlo, y = c // 8, (c // 4) % 2, c % 4
    zhi, core = t // 2, t % 2
    z = zhi * 2 + zlo
    d = own.shape[2]
    half = d // 2
    heads = q.shape[0] // 256
    width = wo.shape[1]
    nchunk = width // d

    def dev(dx=0, dy=0, dz=0, dc=0):
        nx, ny, nz = (x + dx + 4) % 4, (y + dy + 4) % 4, (z + dz + 4) % 4
        return (nx * 8 + (nz % 2) * 4 + ny, (nz // 2) * 2 + (core + dc) % 2)

    right_x, left_x = dev(dx=1), dev(dx=-1)
    right_y, left_y = dev(dy=1), dev(dy=-1)
    up, down = dev(dz=1), dev(dz=-1)
    mate = dev(dc=1)
    zpair = (x * 8 + (1 - zlo) * 4 + y, t)

    wcopies = [
        pltpu.make_async_copy(wq_hbm, wq, wsem.at[0]),
        pltpu.make_async_copy(wk_hbm, wkv.at[:, 0:HEAD], wsem.at[1]),
        pltpu.make_async_copy(wv_hbm, wkv.at[:, HEAD : 2 * HEAD], wsem.at[2]),
        pltpu.make_async_copy(wo_hbm, wo, wsem.at[3]),
    ]
    for copy in wcopies:
        copy.start()

    barrier = pltpu.get_barrier_semaphore()
    for peer in (mate, up, down, right_x, left_x, right_y, left_y):
        pl.semaphore_signal(barrier, inc=1, device_id=peer, device_id_type=MESH)
    pl.semaphore_wait(barrier, 7)

    made = []

    def copy_to(src, dst, peer):
        k = len(made)
        copy = pltpu.make_async_remote_copy(
            src_ref=src, dst_ref=dst, send_sem=ssem.at[k], recv_sem=rsem.at[k],
            device_id=peer, device_id_type=MESH,
        )
        made.append(copy)
        return copy

    to_mate = [copy_to(own.at[b], part.at[b], mate) for b in range(2)]
    to_up = [copy_to(own.at[b, :, 0:half], rel_p.at[b], up) for b in range(2)]
    to_down = [copy_to(own.at[b, :, half:d], rel_m.at[b], down) for b in range(2)]
    fwd_up = [copy_to(rel_p.at[b], zsame.at[b, :, 0:half], up) for b in range(2)]
    fwd_down = [copy_to(rel_m.at[b], zsame.at[b, :, half:d], down) for b in range(2)]
    fwd_mate = [copy_to(zsame.at[b], zother.at[b], mate) for b in range(2)]
    for b in range(2):
        to_up[b].start()
        to_down[b].start()
        to_mate[b].start()

    ssq[...] = jnp.zeros_like(ssq)
    gsum[...] = jnp.zeros_like(gsum)
    src_own, src_mate = t, t + 1 - 2 * core
    src_same = (t + 2) % 4
    src_other = (src_mate + 2) % 4

    def project(ref, b, s, first):
        at = pl.multiple_of(s * d, d)
        rows = pl.ds(at, d)
        ch = ref[b].astype(F32)
        ssq[b] += jnp.broadcast_to(jnp.sum(ch * ch, axis=1, keepdims=True), (BLK, HEAD))
        gsum[b] += jnp.broadcast_to(
            jnp.sum(ch * router[:, rows], axis=1, keepdims=True), (BLK, HEAD)
        )
        cg = (ch * gain[:, rows]).astype(BF)
        pq = dot(cg, wq[rows, :])
        pkv = dot(cg, wkv[rows, :])
        if first:
            qacc[b] = pq
            kvacc[b] = pkv
        else:
            qacc[b] += pq
            kvacc[b] += pkv

    for copy in wcopies[:3]:
        copy.wait()
    for b in range(2):
        project(own, b, src_own, True)
    for b in range(2):
        to_up[b].wait_recv()
        fwd_up[b].start()
        to_down[b].wait_recv()
        fwd_down[b].start()
        if b == 0:
            for bb in range(2):
                to_mate[bb].wait_recv()
                project(part, bb, src_mate, False)
    for b in range(2):
        fwd_up[b].wait_recv()
        fwd_down[b].wait_recv()
        fwd_mate[b].start()
        project(zsame, b, src_same, False)
    for b in range(2):
        fwd_mate[b].wait_recv()
        project(zother, b, src_other, False)

    def rotated(v, b):
        return v * cosf[b] + pltpu.roll(v, HEAD // 2, 1) * sinf[b]

    def unit_at(buf, i, j, k):
        return buf.at[i, pl.ds(pl.multiple_of((j * 2 + k) * BLK, BLK), BLK)]

    def pair_at(buf, i, j):
        return buf.at[i, pl.ds(pl.multiple_of(j * 2 * BLK, 2 * BLK), 2 * BLK)]

    own_a = unit_at(buf_a, y, x, zlo)
    own_b = unit_at(buf_b, x, y, zlo)
    scale = math.log2(math.e) / math.sqrt(HEAD)
    for b, unit in ((0, own_a), (1, own_b)):
        inv = lax.rsqrt(ssq[b][:, 0:1] * (1.0 / width) + norm_eps)
        kv = kvacc[b] * inv
        unit[:, 0:HEAD] = rotated(kv[:, 0:HEAD], b).astype(BF)
        unit[:, HEAD : 2 * HEAD] = kv[:, HEAD:].astype(BF)

    class Side:
        pass

    def side(buf, i, j, plus1, minus1, plus2, minus2):
        s = Side()
        s.buf, s.i, s.j = buf, i, j
        own_unit = unit_at(buf, i, j, zlo)
        s.to_z = copy_to(own_unit, own_unit, zpair)
        z_unit = unit_at(buf, i, j, 1 - zlo)
        s.own_p = copy_to(own_unit, own_unit, plus1)
        s.own_m = copy_to(own_unit, own_unit, minus1)
        s.z_p = copy_to(z_unit, z_unit, plus1)
        s.z_m = copy_to(z_unit, z_unit, minus1)
        jm, jp = (j + 3) % 4, (j + 1) % 4
        s.rel_p = copy_to(unit_at(buf, i, jm, 0), unit_at(buf, i, jm, 0), plus1)
        s.rel_m = copy_to(unit_at(buf, i, jp, 1), unit_at(buf, i, jp, 1), minus1)
        s.order = (j, jm, jp, (j + 2) % 4)
        s.pair_p = [copy_to(pair_at(buf, i, k), pair_at(buf, i, k), plus2) for k in s.order]
        s.pair_m = [copy_to(pair_at(buf, i, k), pair_at(buf, i, k), minus2) for k in s.order]
        im, ip = (i + 3) % 4, (i + 1) % 4
        s.im, s.ip, s.io = im, ip, (i + 2) % 4
        s.opp_p = [copy_to(unit_at(buf, im, k, 0), unit_at(buf, im, k, 0), plus2) for k in s.order]
        s.opp_m = [copy_to(unit_at(buf, ip, k, 1), unit_at(buf, ip, k, 1), minus2) for k in s.order]
        return s

    side_a = side(buf_a, y, x, right_x, left_x, right_y, left_y)
    side_b = side(buf_b, x, y, right_y, left_y, right_x, left_x)
    sides = (side_a, side_b)

    for s in sides:
        s.to_z.start()
        s.own_p.start()
        s.own_m.start()

    for b in range(2):
        inv = lax.rsqrt(ssq[b][:, 0:1] * (1.0 / width) + norm_eps)
        for h in range(heads):
            qh = qacc[b][:, h * HEAD : (h + 1) * HEAD] * inv
            q[h * 256 + b * BLK : h * 256 + (b + 1) * BLK, :] = (
                rotated(qh, b) * scale
            ).astype(BF)

    for s in sides:
        s.to_z.wait_recv()
        s.z_p.start()
        s.z_m.start()
        s.pair_p[0].start()
        s.pair_m[0].start()

    ones_own = jnp.ones((2 * BLK, HEAD), BF)
    keys_own = jnp.concatenate([own_a[...], own_b[...]], axis=0)
    k_own = keys_own[:, 0:HEAD]
    v_own = jnp.concatenate([keys_own[:, HEAD:], ones_own], axis=1)
    row_at = lax.broadcasted_iota(jnp.int32, (256, 256), 0)
    col_at = lax.broadcasted_iota(jnp.int32, (256, 256), 1)
    lower = col_at <= row_at

    def scores_of(qs, ks):
        return lax.dot_general(qs, ks, (((1,), (1,)), ((), ())), preferred_element_type=F32)

    def own_head(h, carry):
        rows = pl.ds(pl.multiple_of(h * 256, 256), 256)
        sc = jnp.where(lower, scores_of(q[rows, :], k_own), LOW)
        high = jnp.max(sc, axis=1, keepdims=True)
        pr = jnp.where(lower, jnp.exp2(sc - high), 0.0).astype(BF)
        m_ref[rows, :] = jnp.broadcast_to(high, (256, HEAD))
        acc[rows, :] = dot(pr, v_own)
        return carry

    lax.fori_loop(0, heads, own_head, 0)

    keys = 8 * BLK
    step_rows = 256

    def attend(buf, g, n, rank_of):
        @pl.when(n > 0)
        def _():
            def rows_step(r, carry):
                rows = pl.ds(pl.multiple_of(r * step_rows, step_rows), step_rows)
                unit_of = lax.broadcasted_iota(jnp.int32, (1, keys), 1) >> 7
                bias = jnp.where(rank_of(unit_of) < n, 0.0, LOW)
                kk = buf[g, :, 0:HEAD]
                vv = jnp.concatenate([buf[g, :, HEAD:], jnp.ones((keys, HEAD), BF)], axis=1)
                sc = scores_of(q[rows, :], kk) + bias
                old = m_ref[rows, :]
                high = jnp.maximum(old, jnp.max(sc, axis=1, keepdims=True))
                pr = jnp.exp2(sc - jnp.concatenate([high] * 8, axis=1)).astype(BF)
                shrink = jnp.exp2(old - high)
                m_ref[rows, :] = high
                acc[rows, :] = acc[rows, :] * jnp.concatenate([shrink] * 2, axis=1) + dot(pr, vv)
                return carry

            lax.fori_loop(0, q.shape[0] // step_rows, rows_step, 0)

    def attend_a(g):
        attend(buf_a, g, x * 2 + zlo + jnp.where(g < y, 1, 0), lambda u: u)

    def attend_b(g):
        count = jnp.where(g < x, 8, jnp.where(g == x, zlo * 4 + y, 0))
        attend(buf_b, g, count, lambda u: (u & 1) * 4 + (u >> 1))

    for s in sides:
        s.own_p.wait_recv()
        s.z_p.wait_recv()
        s.rel_p.start()
        s.own_m.wait_recv()
        s.z_m.wait_recv()
        s.rel_m.start()
        for k in (1, 2):
            s.pair_p[k].start()
            s.pair_m[k].start()
    for s in sides:
        s.rel_p.wait_recv()
        s.rel_m.wait_recv()
        s.pair_p[3].start()
        s.pair_m[3].start()

    def relay(k):
        for s in sides:
            s.pair_p[k].wait_recv()
            s.opp_p[k].start()
            s.pair_m[k].wait_recv()
            s.opp_m[k].start()

    relay(0)
    attend_a(side_a.i)
    relay(1)
    attend_b(side_b.i)
    relay(2)
    relay(3)
    attend_a(side_a.im)
    attend_a(side_a.ip)
    attend_b(side_b.im)
    attend_b(side_b.ip)
    for k in range(4):
        side_a.opp_p[k].wait_recv()
        side_a.opp_m[k].wait_recv()
    attend_a(side_a.io)
    for k in range(4):
        side_b.opp_p[k].wait_recv()
        side_b.opp_m[k].wait_recv()
    attend_b(side_b.io)

    for h in range(heads):
        rows = slice(h * 256, (h + 1) * 256)
        att[:, h * HEAD : (h + 1) * HEAD] = (
            acc[rows, 0:HEAD] / acc[rows, HEAD : 2 * HEAD]
        ).astype(BF)

    wcopies[3].wait()
    piece = BLK // 2
    mine = pl.ds(pl.multiple_of(core * piece, piece), piece)
    other = pl.ds(pl.multiple_of((1 - core) * piece, piece), piece)
    far_rows = pl.ds(pl.multiple_of((1 - zhi) * BLK, BLK), BLK)
    near_rows = pl.ds(pl.multiple_of(zhi * BLK, BLK), BLK)
    order = (0, 2, 1, 3)
    far_mate = [copy_to(d_out.at[j], d_in.at[j], mate) for j in range(4)]
    near_mate = [copy_to(dl_out.at[j], dl_in.at[j], mate) for j in range(4)]
    first_hop = [
        copy_to(zs_out.at[j], zr_rel.at[j], up if j < 2 else down) for j in range(4)
    ]
    second_hop = [
        copy_to(zr_rel.at[j], zr_in.at[j], up if j < 2 else down) for j in range(4)
    ]

    def pass_on(j):
        far_mate[j].wait_recv()
        zs_out[j] = (prem[j, mine, :] + d_in[j].astype(F32)).astype(BF)
        first_hop[j].start()

    last = None
    for j in order:
        prem[j] = dot(att[far_rows, :], wo[:, j * d : (j + 1) * d])
        d_out[j] = prem[j, other, :].astype(BF)
        far_mate[j].start()
        if last is not None:
            pass_on(last)
        last = j
    pass_on(last)
    for k, j in enumerate(order):
        ploc[j] = dot(att[near_rows, :], wo[:, j * d : (j + 1) * d])
        dl_out[j] = ploc[j, other, :].astype(BF)
        near_mate[j].start()
    for j in order:
        first_hop[j].wait_recv()
        second_hop[j].start()
    for j in order:
        near_mate[j].wait_recv()
        ploc[j, mine, :] += dl_in[j].astype(F32)

    gate = 1.0 / (1.0 + jnp.exp(-gsum[zhi, mine, 0:1]))
    for j in order:
        second_hop[j].wait_recv()
    for ref, s in ((own, src_own), (part, src_mate), (zsame, src_same), (zother, src_other)):
        total = ploc[s, mine, :] + zr_in[s].astype(F32)
        out[s] = (ref[zhi, mine, :].astype(F32) + gate * total).astype(BF)

    for copy in made:
        copy.wait_send()


def on_device(resid, sel_blocks, norm_gain, router_weight, w_query, w_key, value_projection, w_out):
    local_rows, d = resid.shape
    width = w_out.shape[1]
    count = local_rows // BLK
    local_ids = sel_blocks - lax.axis_index("ctx") * count
    blocks = resid.reshape(count, BLK, d)
    own = jnp.concatenate(
        [lax.dynamic_slice_in_dim(blocks, local_ids[b], 1, 0) for b in range(2)], axis=0
    )
    positions = sel_blocks[:, None] * BLK + jnp.arange(BLK, dtype=jnp.int32)[None, :]
    freqs = jnp.exp(
        jnp.arange(HEAD // 2, dtype=F32) * (-2.0 * math.log(rope_base) / HEAD)
    )
    angles = positions.astype(F32)[:, :, None] * freqs[None, None, :]
    cosine, sine = jnp.cos(angles), jnp.sin(angles)
    cosf = jnp.concatenate([cosine, cosine], axis=2)
    sinf = jnp.concatenate([-sine, sine], axis=2)
    qcols = w_query.shape[1]
    heads = qcols // HEAD
    vmem = pl.BlockSpec(memory_space=pltpu.VMEM)
    anyspace = pl.BlockSpec(memory_space=pl.ANY)
    piece = BLK // 2
    nsem = 74
    result = pl.pallas_call(
        layer_kernel,
        name="layer",
        out_shape=jax.ShapeDtypeStruct((4, piece, d), BF),
        in_specs=[vmem] * 5 + [anyspace] * 4,
        out_specs=vmem,
        scratch_shapes=[
            pltpu.VMEM((width, qcols), BF),
            pltpu.VMEM((width, 2 * HEAD), BF),
            pltpu.VMEM((qcols, width), BF),
            pltpu.VMEM((2, BLK, d), BF),
            pltpu.VMEM((2, BLK, d), BF),
            pltpu.VMEM((2, BLK, d), BF),
            pltpu.VMEM((2, BLK, d // 2), BF),
            pltpu.VMEM((2, BLK, d // 2), BF),
            pltpu.VMEM((2, BLK, qcols), F32),
            pltpu.VMEM((2, BLK, 2 * HEAD), F32),
            pltpu.VMEM((2, BLK, HEAD), F32),
            pltpu.VMEM((2, BLK, HEAD), F32),
            pltpu.VMEM((heads * 256, HEAD), BF),
            pltpu.VMEM((4, 8 * BLK, 2 * HEAD), BF),
            pltpu.VMEM((4, 8 * BLK, 2 * HEAD), BF),
            pltpu.VMEM((heads * 256, HEAD), F32),
            pltpu.VMEM((heads * 256, 2 * HEAD), F32),
            pltpu.VMEM((256, qcols), BF),
            pltpu.VMEM((4, BLK, d), F32),
            pltpu.VMEM((4, BLK, d), F32),
            pltpu.VMEM((4, piece, d), BF),
            pltpu.VMEM((4, piece, d), BF),
            pltpu.VMEM((4, piece, d), BF),
            pltpu.VMEM((4, piece, d), BF),
            pltpu.VMEM((4, piece, d), BF),
            pltpu.VMEM((4, piece, d), BF),
            pltpu.VMEM((4, piece, d), BF),
            pltpu.SemaphoreType.DMA((nsem,)),
            pltpu.SemaphoreType.DMA((nsem,)),
            pltpu.SemaphoreType.DMA((4,)),
        ],
        compiler_params=pltpu.CompilerParams(
            collective_id=0, has_side_effects=True, vmem_limit_bytes=60 * 1024 * 1024
        ),
    )(
        own, cosf, sinf, norm_gain.reshape(1, width), router_weight.reshape(1, width),
        w_query, w_key, value_projection, w_out,
    )
    return result.transpose(1, 0, 2).reshape(piece, width)


def solution(mesh):
    return jax.shard_map(
        on_device,
        mesh=mesh,
        in_specs=(
            P("ctx", "tp"),
            P("ctx"),
            P(),
            P(),
            P(None, "tp"),
            P(None, "tp"),
            P(None, "tp"),
            P("tp", None),
        ),
        out_specs=P(("ctx", "tp"), None),
        check_vma=False,
    )
```

```python
import math

import jax
import jax.numpy as jnp
from jax import lax
from jax.experimental import pallas as pl
from jax.experimental.pallas import tpu as pltpu
from jax.sharding import PartitionSpec as P

HEAD = 128
BLK = 128
MESH = pl.DeviceIdType.MESH
BF = jnp.bfloat16
F32 = jnp.float32

rope_base = 500000.0
norm_eps = 1e-05
LOW = -1e30


def dot(a, b):
    return jnp.dot(a, b, preferred_element_type=F32)


def layer_kernel(
    own, cosf, sinf, gain, router, wq_hbm, wk_hbm, wv_hbm, wo_hbm,
    out,
    wq, wkv, wo, part, zsame, zother, rel_p, rel_m,
    qacc, kvacc, ssq, gsum, q, buf, m_ref, acc, s_ref, p_ref, x_ref, att,
    prem, ploc, d_out, d_in, dl_out, dl_in, zs_out, zr_rel, zr_in,
    ssem, rsem, wsem,
):
    c = lax.axis_index("ctx")
    t = lax.axis_index("tp")
    x, zlo, y = c // 8, (c // 4) % 2, c % 4
    zhi, core = t // 2, t % 2
    z = zhi * 2 + zlo
    d = own.shape[2]
    half = d // 2
    heads = q.shape[0] // 256
    width = wo.shape[1]
    nchunk = width // d

    def dev(dx=0, dy=0, dz=0, dc=0):
        nx, ny, nz = (x + dx + 4) % 4, (y + dy + 4) % 4, (z + dz + 4) % 4
        return (nx * 8 + (nz % 2) * 4 + ny, (nz // 2) * 2 + (core + dc) % 2)

    right_x, left_x = dev(dx=1), dev(dx=-1)
    right_y, left_y = dev(dy=1), dev(dy=-1)
    up, down = dev(dz=1), dev(dz=-1)
    mate = dev(dc=1)
    zpair = (x * 8 + (1 - zlo) * 4 + y, t)

    wcopies = [
        pltpu.make_async_copy(wq_hbm, wq, wsem.at[0]),
        pltpu.make_async_copy(wk_hbm, wkv.at[:, 0:HEAD], wsem.at[1]),
        pltpu.make_async_copy(wv_hbm, wkv.at[:, HEAD : 2 * HEAD], wsem.at[2]),
        pltpu.make_async_copy(wo_hbm, wo, wsem.at[3]),
    ]
    for copy in wcopies:
        copy.start()

    barrier = pltpu.get_barrier_semaphore()
    for peer in (mate, up, down, right_x, left_x, right_y, left_y):
        pl.semaphore_signal(barrier, inc=1, device_id=peer, device_id_type=MESH)
    pl.semaphore_wait(barrier, 7)

    made = []

    def copy_to(src, dst, peer):
        k = len(made)
        copy = pltpu.make_async_remote_copy(
            src_ref=src, dst_ref=dst, send_sem=ssem.at[k], recv_sem=rsem.at[k],
            device_id=peer, device_id_type=MESH,
        )
        made.append(copy)
        return copy

    to_mate = [copy_to(own.at[b], part.at[b], mate) for b in range(2)]
    to_up = [copy_to(own.at[b, :, 0:half], rel_p.at[b], up) for b in range(2)]
    to_down = [copy_to(own.at[b, :, half:d], rel_m.at[b], down) for b in range(2)]
    fwd_up = [copy_to(rel_p.at[b], zsame.at[b, :, 0:half], up) for b in range(2)]
    fwd_down = [copy_to(rel_m.at[b], zsame.at[b, :, half:d], down) for b in range(2)]
    fwd_mate = [copy_to(zsame.at[b], zother.at[b], mate) for b in range(2)]
    for b in range(2):
        to_up[b].start()
        to_down[b].start()
        to_mate[b].start()

    ssq[...] = jnp.zeros_like(ssq)
    gsum[...] = jnp.zeros_like(gsum)
    src_own, src_mate = t, t + 1 - 2 * core
    src_same = (t + 2) % 4
    src_other = (src_mate + 2) % 4

    def project(ref, b, s, first):
        at = pl.multiple_of(s * d, d)
        rows = pl.ds(at, d)
        ch = ref[b].astype(F32)
        ssq[b] += jnp.broadcast_to(jnp.sum(ch * ch, axis=1, keepdims=True), (BLK, HEAD))
        gsum[b] += jnp.broadcast_to(
            jnp.sum(ch * router[:, rows], axis=1, keepdims=True), (BLK, HEAD)
        )
        cg = (ch * gain[:, rows]).astype(BF)
        pq = dot(cg, wq[rows, :])
        pkv = dot(cg, wkv[rows, :])
        if first:
            qacc[b] = pq
            kvacc[b] = pkv
        else:
            qacc[b] += pq
            kvacc[b] += pkv

    for copy in wcopies[:3]:
        copy.wait()
    for b in range(2):
        project(own, b, src_own, True)
    for b in range(2):
        to_up[b].wait_recv()
        fwd_up[b].start()
        to_down[b].wait_recv()
        fwd_down[b].start()
        if b == 0:
            for bb in range(2):
                to_mate[bb].wait_recv()
                project(part, bb, src_mate, False)
    for b in range(2):
        fwd_up[b].wait_recv()
        fwd_down[b].wait_recv()
        fwd_mate[b].start()
        project(zsame, b, src_same, False)
    for b in range(2):
        fwd_mate[b].wait_recv()
        project(zother, b, src_other, False)

    def rotated(v, b):
        return v * cosf[b] + pltpu.roll(v, HEAD // 2, 1) * sinf[b]

    def unit_at(base, i, j, k):
        return buf.at[base + i, pl.ds(pl.multiple_of((j * 2 + k) * BLK, BLK), BLK)]

    def pair_at(base, i, j):
        return buf.at[base + i, pl.ds(pl.multiple_of(j * 2 * BLK, 2 * BLK), 2 * BLK)]

    own_a = unit_at(0, y, x, zlo)
    own_b = unit_at(4, x, y, zlo)
    scale = math.log2(math.e) / math.sqrt(HEAD)
    for b, unit in ((0, own_a), (1, own_b)):
        inv = lax.rsqrt(ssq[b][:, 0:1] * (1.0 / width) + norm_eps)
        kv = kvacc[b] * inv
        unit[:, 0:HEAD] = rotated(kv[:, 0:HEAD], b).astype(BF)
        unit[:, HEAD : 2 * HEAD] = kv[:, HEAD:].T.astype(BF)

    class Side:
        pass

    def side(base, i, j, plus1, minus1, plus2, minus2):
        s = Side()
        own_unit = unit_at(base, i, j, zlo)
        s.to_z = copy_to(own_unit, own_unit, zpair)
        z_unit = unit_at(base, i, j, 1 - zlo)
        s.own_p = copy_to(own_unit, own_unit, plus1)
        s.own_m = copy_to(own_unit, own_unit, minus1)
        s.z_p = copy_to(z_unit, z_unit, plus1)
        s.z_m = copy_to(z_unit, z_unit, minus1)
        jm, jp = (j + 3) % 4, (j + 1) % 4
        s.rel_p = copy_to(unit_at(base, i, jm, 0), unit_at(base, i, jm, 0), plus1)
        s.rel_m = copy_to(unit_at(base, i, jp, 1), unit_at(base, i, jp, 1), minus1)
        s.order = (j, jm, jp, (j + 2) % 4)
        s.pair_p = [copy_to(pair_at(base, i, k), pair_at(base, i, k), plus2) for k in s.order]
        s.pair_m = [copy_to(pair_at(base, i, k), pair_at(base, i, k), minus2) for k in s.order]
        im, ip = (i + 3) % 4, (i + 1) % 4
        s.i, s.im, s.ip, s.io = i, im, ip, (i + 2) % 4
        s.opp_p = [copy_to(unit_at(base, im, k, 0), unit_at(base, im, k, 0), plus2) for k in s.order]
        s.opp_m = [copy_to(unit_at(base, ip, k, 1), unit_at(base, ip, k, 1), minus2) for k in s.order]
        return s

    side_a = side(0, y, x, right_x, left_x, right_y, left_y)
    side_b = side(4, x, y, right_y, left_y, right_x, left_x)
    sides = (side_a, side_b)

    for s in sides:
        s.to_z.start()
        s.own_p.start()
        s.own_m.start()

    for b in range(2):
        inv = lax.rsqrt(ssq[b][:, 0:1] * (1.0 / width) + norm_eps)
        for h in range(heads):
            qh = qacc[b][:, h * HEAD : (h + 1) * HEAD] * inv
            q[h * 256 + b * BLK : h * 256 + (b + 1) * BLK, :] = (
                rotated(qh, b) * scale
            ).astype(BF)

    for s in sides:
        s.to_z.wait_recv()
        s.z_p.start()
        s.z_m.start()
        s.pair_p[0].start()
        s.pair_m[0].start()

    cols = 512
    tiles = heads * 256 // cols
    ones_rows = jnp.ones((16, 8 * BLK), BF)

    def scores_of(ks, r):
        return lax.dot_general(
            ks, q[r * cols : (r + 1) * cols, :], (((1,), (1,)), ((), ())),
            preferred_element_type=F32,
        )

    keys_own = jnp.concatenate([own_a[:, 0:HEAD], own_b[:, 0:HEAD]], axis=0)
    v_own = jnp.concatenate([own_a[:, HEAD:], own_b[:, HEAD:]], axis=1)
    v_own = jnp.concatenate([v_own, ones_rows[:, 0 : 2 * BLK]], axis=0)
    key_at = lax.broadcasted_iota(jnp.int32, (256, cols), 0)
    query_at = lax.broadcasted_iota(jnp.int32, (256, cols), 1) & 255
    upper = key_at <= query_at
    for r in range(tiles):
        at = slice(r * cols, (r + 1) * cols)
        sc = jnp.where(upper, scores_of(keys_own, r), LOW)
        high = jnp.max(sc, axis=0, keepdims=True)
        pr = jnp.where(upper, jnp.exp2(sc - high), 0.0).astype(BF)
        m_ref[:, at] = jnp.broadcast_to(high, (8, cols))
        acc[:, at] = dot(v_own, pr)

    def attend(g, n, rank):
        @pl.when(n > 0)
        def _():
            def score(r):
                sc = scores_of(buf[g, :, 0:HEAD], r)
                s_ref[r % 2] = jnp.concatenate(
                    [
                        sc[u * BLK : (u + 1) * BLK] + jnp.where(rank(u) < n, 0.0, LOW)
                        for u in range(8)
                    ],
                    axis=0,
                )

            def soften(r):
                at = slice(r * cols, (r + 1) * cols)
                sc = s_ref[r % 2]
                old = m_ref[0:1, at]
                high = jnp.maximum(old, jnp.max(sc, axis=0, keepdims=True))
                p_ref[r % 2] = jnp.exp2(sc - high).astype(BF)
                x_ref[r % 2] = jnp.broadcast_to(jnp.exp2(old - high), (8, cols))
                m_ref[:, at] = jnp.broadcast_to(high, (8, cols))

            def collect(r):
                at = slice(r * cols, (r + 1) * cols)
                vt = jnp.concatenate(
                    [buf[g, u * BLK : (u + 1) * BLK, HEAD:] for u in range(8)], axis=1
                )
                vt = jnp.concatenate([vt, ones_rows], axis=0)
                acc[:, at] = acc[:, at] * x_ref[r % 2][0:1] + dot(vt, p_ref[r % 2])

            for k in range(tiles + 2):
                if k < tiles:
                    score(k)
                if k >= 2:
                    collect(k - 2)
                if 1 <= k <= tiles:
                    soften(k - 1)

    def attend_a(g):
        attend(g, x * 2 + zlo + jnp.where(g < y, 1, 0), lambda u: u)

    def attend_b(g):
        count = jnp.where(g < x, 8, jnp.where(g == x, zlo * 4 + y, 0))
        attend(4 + g, count, lambda u: (u & 1) * 4 + (u >> 1))

    for s in sides:
        s.own_p.wait_recv()
        s.z_p.wait_recv()
        s.rel_p.start()
        s.own_m.wait_recv()
        s.z_m.wait_recv()
        s.rel_m.start()
        for k in (1, 2):
            s.pair_p[k].start()
            s.pair_m[k].start()
    for s in sides:
        s.rel_p.wait_recv()
        s.rel_m.wait_recv()
        s.pair_p[3].start()
        s.pair_m[3].start()

    def relay(k):
        for s in sides:
            s.pair_p[k].wait_recv()
            s.opp_p[k].start()
            s.pair_m[k].wait_recv()
            s.opp_m[k].start()

    relay(0)
    attend_a(side_a.i)
    relay(1)
    attend_b(side_b.i)
    relay(2)
    relay(3)

    def both_a(k, carry):
        attend_a(lax.rem(y + 3 + 2 * k, 4))
        return carry

    def both_b(k, carry):
        attend_b(lax.rem(x + 3 + 2 * k, 4))
        return carry

    lax.fori_loop(0, 2, both_a, 0)
    lax.fori_loop(0, 2, both_b, 0)
    for k in range(4):
        side_a.opp_p[k].wait_recv()
        side_a.opp_m[k].wait_recv()
    attend_a(side_a.io)
    for k in range(4):
        side_b.opp_p[k].wait_recv()
        side_b.opp_m[k].wait_recv()
    attend_b(side_b.io)

    for h in range(heads):
        at = slice(h * 256, (h + 1) * 256)
        att[:, h * HEAD : (h + 1) * HEAD] = (
            (acc[0:HEAD, at] / acc[HEAD : HEAD + 1, at]).T
        ).astype(BF)

    wcopies[3].wait()
    piece = BLK // 2
    mine = pl.ds(pl.multiple_of(core * piece, piece), piece)
    other = pl.ds(pl.multiple_of((1 - core) * piece, piece), piece)
    far_rows = pl.ds(pl.multiple_of((1 - zhi) * BLK, BLK), BLK)
    near_rows = pl.ds(pl.multiple_of(zhi * BLK, BLK), BLK)
    order = (0, 2, 1, 3)
    far_mate = [copy_to(d_out.at[j], d_in.at[j], mate) for j in range(4)]
    near_mate = [copy_to(dl_out.at[j], dl_in.at[j], mate) for j in range(4)]
    first_hop = [
        copy_to(zs_out.at[j], zr_rel.at[j], up if j < 2 else down) for j in range(4)
    ]
    second_hop = [
        copy_to(zr_rel.at[j], zr_in.at[j], up if j < 2 else down) for j in range(4)
    ]

    def pass_on(j):
        far_mate[j].wait_recv()
        zs_out[j] = (prem[j, mine, :] + d_in[j].astype(F32)).astype(BF)
        first_hop[j].start()

    last = None
    for j in order:
        prem[j] = dot(att[far_rows, :], wo[:, j * d : (j + 1) * d])
        d_out[j] = prem[j, other, :].astype(BF)
        far_mate[j].start()
        if last is not None:
            pass_on(last)
        last = j
    pass_on(last)
    for k, j in enumerate(order):
        ploc[j] = dot(att[near_rows, :], wo[:, j * d : (j + 1) * d])
        dl_out[j] = ploc[j, other, :].astype(BF)
        near_mate[j].start()
    for j in order:
        first_hop[j].wait_recv()
        second_hop[j].start()
    for j in order:
        near_mate[j].wait_recv()
        ploc[j, mine, :] += dl_in[j].astype(F32)

    gate = 1.0 / (1.0 + jnp.exp(-gsum[zhi, mine, 0:1]))
    for j in order:
        second_hop[j].wait_recv()
    for ref, s in ((own, src_own), (part, src_mate), (zsame, src_same), (zother, src_other)):
        total = ploc[s, mine, :] + zr_in[s].astype(F32)
        out[s] = (ref[zhi, mine, :].astype(F32) + gate * total).astype(BF)

    for copy in made:
        copy.wait_send()


def on_device(resid, sel_blocks, norm_gain, router_weight, w_query, w_key, value_projection, w_out):
    local_rows, d = resid.shape
    width = w_out.shape[1]
    count = local_rows // BLK
    local_ids = sel_blocks - lax.axis_index("ctx") * count
    blocks = resid.reshape(count, BLK, d)
    own = jnp.concatenate(
        [lax.dynamic_slice_in_dim(blocks, local_ids[b], 1, 0) for b in range(2)], axis=0
    )
    positions = sel_blocks[:, None] * BLK + jnp.arange(BLK, dtype=jnp.int32)[None, :]
    freqs = jnp.exp(
        jnp.arange(HEAD // 2, dtype=F32) * (-2.0 * math.log(rope_base) / HEAD)
    )
    angles = positions.astype(F32)[:, :, None] * freqs[None, None, :]
    cosine, sine = jnp.cos(angles), jnp.sin(angles)
    cosf = jnp.concatenate([cosine, cosine], axis=2)
    sinf = jnp.concatenate([-sine, sine], axis=2)
    qcols = w_query.shape[1]
    heads = qcols // HEAD
    vmem = pl.BlockSpec(memory_space=pltpu.VMEM)
    anyspace = pl.BlockSpec(memory_space=pl.ANY)
    piece = BLK // 2
    nsem = 74
    result = pl.pallas_call(
        layer_kernel,
        name="layer",
        out_shape=jax.ShapeDtypeStruct((4, piece, d), BF),
        in_specs=[vmem] * 5 + [anyspace] * 4,
        out_specs=vmem,
        scratch_shapes=[
            pltpu.VMEM((width, qcols), BF),
            pltpu.VMEM((width, 2 * HEAD), BF),
            pltpu.VMEM((qcols, width), BF),
            pltpu.VMEM((2, BLK, d), BF),
            pltpu.VMEM((2, BLK, d), BF),
            pltpu.VMEM((2, BLK, d), BF),
            pltpu.VMEM((2, BLK, d // 2), BF),
            pltpu.VMEM((2, BLK, d // 2), BF),
            pltpu.VMEM((2, BLK, qcols), F32),
            pltpu.VMEM((2, BLK, 2 * HEAD), F32),
            pltpu.VMEM((2, BLK, HEAD), F32),
            pltpu.VMEM((2, BLK, HEAD), F32),
            pltpu.VMEM((heads * 256, HEAD), BF),
            pltpu.VMEM((8, 8 * BLK, 2 * HEAD), BF),
            pltpu.VMEM((8, heads * 256), F32),
            pltpu.VMEM((HEAD + 16, heads * 256), F32),
            pltpu.VMEM((2, 8 * BLK, 512), F32),
            pltpu.VMEM((2, 8 * BLK, 512), BF),
            pltpu.VMEM((2, 8, 512), F32),
            pltpu.VMEM((256, qcols), BF),
            pltpu.VMEM((4, BLK, d), F32),
            pltpu.VMEM((4, BLK, d), F32),
            pltpu.VMEM((4, piece, d), BF),
            pltpu.VMEM((4, piece, d), BF),
            pltpu.VMEM((4, piece, d), BF),
            pltpu.VMEM((4, piece, d), BF),
            pltpu.VMEM((4, piece, d), BF),
            pltpu.VMEM((4, piece, d), BF),
            pltpu.VMEM((4, piece, d), BF),
            pltpu.SemaphoreType.DMA((nsem,)),
            pltpu.SemaphoreType.DMA((nsem,)),
            pltpu.SemaphoreType.DMA((4,)),
        ],
        compiler_params=pltpu.CompilerParams(
            collective_id=0, has_side_effects=True, vmem_limit_bytes=60 * 1024 * 1024
        ),
    )(
        own, cosf, sinf, norm_gain.reshape(1, width), router_weight.reshape(1, width),
        w_query, w_key, value_projection, w_out,
    )
    return result.transpose(1, 0, 2).reshape(piece, width)


def solution(mesh):
    return jax.shard_map(
        on_device,
        mesh=mesh,
        in_specs=(
            P("ctx", "tp"),
            P("ctx"),
            P(),
            P(),
            P(None, "tp"),
            P(None, "tp"),
            P(None, "tp"),
            P("tp", None),
        ),
        out_specs=P(("ctx", "tp"), None),
        check_vma=False,
    )
```

```python
import math

import jax
import jax.numpy as jnp
from jax import lax
from jax.experimental import pallas as pl
from jax.experimental.pallas import tpu as pltpu
from jax.sharding import PartitionSpec as P

HEAD = 128
BLK = 128
MESH = pl.DeviceIdType.MESH
BF = jnp.bfloat16
F32 = jnp.float32

rope_base = 500000.0
norm_eps = 1e-05
LOW = -1e30


def dot(a, b):
    return jnp.dot(a, b, preferred_element_type=F32)


def layer_kernel(
    sel, freq, gain, router, resid_hbm, wq_hbm, wk_hbm, wv_hbm, wo_hbm,
    out,
    resid, own, cosf, sinf, wq, wkv, wo, part, zsame, zother, rel_p, rel_m,
    qacc, kvacc, ssq, gsum, q, buf, m_ref, acc, s_ref, p_ref, x_ref, att,
    prem, ploc, d_out, d_in, dl_out, dl_in, zs_out, zr_rel, zr_in,
    ssem, rsem, wsem,
):
    c = lax.axis_index("ctx")
    t = lax.axis_index("tp")
    x, zlo, y = c // 8, (c // 4) % 2, c % 4
    zhi, core = t // 2, t % 2
    z = zhi * 2 + zlo
    d = own.shape[2]
    half = d // 2
    heads = q.shape[0] // 256
    width = wo.shape[1]
    nchunk = width // d

    def dev(dx=0, dy=0, dz=0, dc=0):
        nx, ny, nz = (x + dx + 4) % 4, (y + dy + 4) % 4, (z + dz + 4) % 4
        return (nx * 8 + (nz % 2) * 4 + ny, (nz // 2) * 2 + (core + dc) % 2)

    right_x, left_x = dev(dx=1), dev(dx=-1)
    right_y, left_y = dev(dy=1), dev(dy=-1)
    up, down = dev(dz=1), dev(dz=-1)
    mate = dev(dc=1)
    zpair = (x * 8 + (1 - zlo) * 4 + y, t)

    wcopies = [
        pltpu.make_async_copy(wq_hbm, wq, wsem.at[0]),
        pltpu.make_async_copy(wk_hbm, wkv.at[:, 0:HEAD], wsem.at[1]),
        pltpu.make_async_copy(wv_hbm, wkv.at[:, HEAD : 2 * HEAD], wsem.at[2]),
        pltpu.make_async_copy(wo_hbm, wo, wsem.at[3]),
    ]
    rcopy = pltpu.make_async_copy(resid_hbm, resid, wsem.at[4])
    rcopy.start()
    for copy in wcopies:
        copy.start()

    barrier = pltpu.get_barrier_semaphore()
    for peer in (mate, up, down, right_x, left_x, right_y, left_y):
        pl.semaphore_signal(barrier, inc=1, device_id=peer, device_id_type=MESH)
    rcopy.wait()
    for b in range(2):
        at = jnp.clip(sel[b] - c * resid.shape[0], 0, resid.shape[0] - 1)
        own[b] = resid[at]
    pl.semaphore_wait(barrier, 7)

    made = []

    def copy_to(src, dst, peer):
        k = len(made)
        copy = pltpu.make_async_remote_copy(
            src_ref=src, dst_ref=dst, send_sem=ssem.at[k], recv_sem=rsem.at[k],
            device_id=peer, device_id_type=MESH,
        )
        made.append(copy)
        return copy

    to_mate = [copy_to(own.at[b], part.at[b], mate) for b in range(2)]
    to_up = [copy_to(own.at[b, :, 0:half], rel_p.at[b], up) for b in range(2)]
    to_down = [copy_to(own.at[b, :, half:d], rel_m.at[b], down) for b in range(2)]
    fwd_up = [copy_to(rel_p.at[b], zsame.at[b, :, 0:half], up) for b in range(2)]
    fwd_down = [copy_to(rel_m.at[b], zsame.at[b, :, half:d], down) for b in range(2)]
    fwd_mate = [copy_to(zsame.at[b], zother.at[b], mate) for b in range(2)]
    for b in range(2):
        to_up[b].start()
        to_down[b].start()
        to_mate[b].start()

    lane = lax.broadcasted_iota(jnp.int32, (BLK, HEAD), 1)
    row = lax.broadcasted_iota(jnp.int32, (BLK, HEAD), 0)
    for b in range(2):
        angle = (row + sel[b] * BLK).astype(F32) * freq[...]
        cosf[b] = jnp.cos(angle)
        sine = jnp.sin(angle)
        sinf[b] = jnp.where(lane < HEAD // 2, -sine, sine)
    ssq[...] = jnp.zeros_like(ssq)
    gsum[...] = jnp.zeros_like(gsum)
    src_own, src_mate = t, t + 1 - 2 * core
    src_same = (t + 2) % 4
    src_other = (src_mate + 2) % 4

    def project(ref, b, s, first):
        at = pl.multiple_of(s * d, d)
        rows = pl.ds(at, d)
        ch = ref[b].astype(F32)
        ssq[b] += jnp.broadcast_to(jnp.sum(ch * ch, axis=1, keepdims=True), (BLK, HEAD))
        gsum[b] += jnp.broadcast_to(
            jnp.sum(ch * router[:, rows], axis=1, keepdims=True), (BLK, HEAD)
        )
        cg = (ch * gain[:, rows]).astype(BF)
        pq = dot(cg, wq[rows, :])
        pkv = dot(cg, wkv[rows, :])
        if first:
            qacc[b] = pq
            kvacc[b] = pkv
        else:
            qacc[b] += pq
            kvacc[b] += pkv

    for copy in wcopies[:3]:
        copy.wait()
    for b in range(2):
        project(own, b, src_own, True)
    for b in range(2):
        to_up[b].wait_recv()
        fwd_up[b].start()
        to_down[b].wait_recv()
        fwd_down[b].start()
        if b == 0:
            for bb in range(2):
                to_mate[bb].wait_recv()
                project(part, bb, src_mate, False)
    for b in range(2):
        fwd_up[b].wait_recv()
        fwd_down[b].wait_recv()
        fwd_mate[b].start()
        project(zsame, b, src_same, False)
    for b in range(2):
        fwd_mate[b].wait_recv()
        project(zother, b, src_other, False)

    def rotated(v, b):
        return v * cosf[b] + pltpu.roll(v, HEAD // 2, 1) * sinf[b]

    def unit_at(base, i, j, k):
        return buf.at[base + i, pl.ds(pl.multiple_of((j * 2 + k) * BLK, BLK), BLK)]

    def pair_at(base, i, j):
        return buf.at[base + i, pl.ds(pl.multiple_of(j * 2 * BLK, 2 * BLK), 2 * BLK)]

    own_a = unit_at(0, y, x, zlo)
    own_b = unit_at(4, x, y, zlo)
    scale = math.log2(math.e) / math.sqrt(HEAD)
    for b, unit in ((0, own_a), (1, own_b)):
        inv = lax.rsqrt(ssq[b][:, 0:1] * (1.0 / width) + norm_eps)
        kv = kvacc[b] * inv
        unit[:, 0:HEAD] = rotated(kv[:, 0:HEAD], b).astype(BF)
        unit[:, HEAD : 2 * HEAD] = kv[:, HEAD:].T.astype(BF)

    class Side:
        pass

    def side(base, i, j, plus1, minus1, plus2, minus2):
        s = Side()
        own_unit = unit_at(base, i, j, zlo)
        s.to_z = copy_to(own_unit, own_unit, zpair)
        z_unit = unit_at(base, i, j, 1 - zlo)
        s.own_p = copy_to(own_unit, own_unit, plus1)
        s.own_m = copy_to(own_unit, own_unit, minus1)
        s.z_p = copy_to(z_unit, z_unit, plus1)
        s.z_m = copy_to(z_unit, z_unit, minus1)
        jm, jp = (j + 3) % 4, (j + 1) % 4
        s.rel_p = copy_to(unit_at(base, i, jm, 0), unit_at(base, i, jm, 0), plus1)
        s.rel_m = copy_to(unit_at(base, i, jp, 1), unit_at(base, i, jp, 1), minus1)
        s.order = (j, jm, jp, (j + 2) % 4)
        s.pair_p = [copy_to(pair_at(base, i, k), pair_at(base, i, k), plus2) for k in s.order]
        s.pair_m = [copy_to(pair_at(base, i, k), pair_at(base, i, k), minus2) for k in s.order]
        im, ip = (i + 3) % 4, (i + 1) % 4
        s.base, s.i, s.j, s.im, s.ip, s.io = base, i, j, im, ip, (i + 2) % 4
        s.opp_p = [copy_to(unit_at(base, im, k, 0), unit_at(base, im, k, 0), plus2) for k in s.order]
        s.opp_m = [copy_to(unit_at(base, ip, k, 1), unit_at(base, ip, k, 1), minus2) for k in s.order]
        return s

    side_a = side(0, y, x, right_x, left_x, right_y, left_y)
    side_b = side(4, x, y, right_y, left_y, right_x, left_x)
    sides = (side_a, side_b)

    for s in sides:
        s.to_z.start()
        s.own_p.start()
        s.own_m.start()

    for b in range(2):
        inv = lax.rsqrt(ssq[b][:, 0:1] * (1.0 / width) + norm_eps)
        for h in range(heads):
            qh = qacc[b][:, h * HEAD : (h + 1) * HEAD] * inv
            q[h * 256 + b * BLK : h * 256 + (b + 1) * BLK, :] = (
                rotated(qh, b) * scale
            ).astype(BF)

    for s in sides:
        s.to_z.wait_recv()
        s.z_p.start()
        s.z_m.start()
        s.pair_p[0].start()
        s.pair_m[0].start()

    cols = 512
    tiles = heads * 256 // cols
    ones_rows = jnp.ones((16, 8 * BLK), BF)

    def scores_of(ks, r):
        return lax.dot_general(
            ks, q[r * cols : (r + 1) * cols, :], (((1,), (1,)), ((), ())),
            preferred_element_type=F32,
        )

    keys_own = jnp.concatenate([own_a[:, 0:HEAD], own_b[:, 0:HEAD]], axis=0)
    v_own = jnp.concatenate([own_a[:, HEAD:], own_b[:, HEAD:]], axis=1)
    v_own = jnp.concatenate([v_own, ones_rows[:, 0 : 2 * BLK]], axis=0)
    key_at = lax.broadcasted_iota(jnp.int32, (256, cols), 0)
    query_at = lax.broadcasted_iota(jnp.int32, (256, cols), 1) & 255
    upper = key_at <= query_at
    for r in range(tiles):
        at = slice(r * cols, (r + 1) * cols)
        sc = jnp.where(upper, scores_of(keys_own, r), LOW)
        high = jnp.max(sc, axis=0, keepdims=True)
        pr = jnp.where(upper, jnp.exp2(sc - high), 0.0).astype(BF)
        m_ref[:, at] = jnp.broadcast_to(high, (8, cols))
        acc[:, at] = dot(v_own, pr)

    def attend(pairs):
        allowed = []
        for base, i, j in pairs:
            for k in range(2):
                place = i * 8 + j if base else j * 8 + i
                allowed.append(place + k * 4 < c)
        some = allowed[0]
        for flag in allowed[1:]:
            some = jnp.logical_or(some, flag)

        @pl.when(some)
        def _():
            def score(r):
                ks = jnp.concatenate([pair_at(*pr)[:, 0:HEAD] for pr in pairs], axis=0)
                sc = scores_of(ks, r)
                s_ref[r % 2] = jnp.concatenate(
                    [
                        sc[u * BLK : (u + 1) * BLK] + jnp.where(allowed[u], 0.0, LOW)
                        for u in range(8)
                    ],
                    axis=0,
                )

            def soften(r):
                at = slice(r * cols, (r + 1) * cols)
                sc = s_ref[r % 2]
                old = m_ref[0:1, at]
                high = jnp.maximum(old, jnp.max(sc, axis=0, keepdims=True))
                p_ref[r % 2] = jnp.exp2(sc - high).astype(BF)
                x_ref[r % 2] = jnp.broadcast_to(jnp.exp2(old - high), (8, cols))
                m_ref[:, at] = jnp.broadcast_to(high, (8, cols))

            def collect(r):
                at = slice(r * cols, (r + 1) * cols)
                vt = jnp.concatenate(
                    [unit_at(*pr, k)[:, HEAD:] for pr in pairs for k in range(2)], axis=1
                )
                vt = jnp.concatenate([vt, ones_rows], axis=0)
                acc[:, at] = acc[:, at] * x_ref[r % 2][0:1] + dot(vt, p_ref[r % 2])

            for k in range(tiles + 2):
                if k < tiles:
                    score(k)
                if k >= 2:
                    collect(k - 2)
                if 1 <= k <= tiles:
                    soften(k - 1)

    def attend_own(k0, k1):
        attend([(s.base, s.i, s.order[k]) for s in sides for k in (k0, k1)])

    def attend_near(step):
        attend([(s.base, g, lax.rem(s.j + step, 4)) for s in sides for g in (s.im, s.ip)])

    def attend_far(k0, k1):
        for s in sides:
            for k in (k0, k1):
                s.opp_p[k].wait_recv()
                s.opp_m[k].wait_recv()
        attend([(s.base, s.io, s.order[k]) for s in sides for k in (k0, k1)])

    for s in sides:
        s.own_p.wait_recv()
        s.z_p.wait_recv()
        s.rel_p.start()
        s.own_m.wait_recv()
        s.z_m.wait_recv()
        s.rel_m.start()
        for k in (1, 2):
            s.pair_p[k].start()
            s.pair_m[k].start()
    attend_own(0, 1)
    for s in sides:
        s.rel_p.wait_recv()
        s.rel_m.wait_recv()
        s.pair_p[3].start()
        s.pair_m[3].start()

    def relay(k):
        for s in sides:
            s.pair_p[k].wait_recv()
            s.opp_p[k].start()
            s.pair_m[k].wait_recv()
            s.opp_m[k].start()

    relay(0)
    attend_own(2, 3)
    relay(1)
    attend_near(0)
    relay(2)
    attend_near(3)
    relay(3)

    def near_step(k, carry):
        attend_near(k)
        return carry

    lax.fori_loop(1, 3, near_step, 0)
    attend_far(0, 1)
    attend_far(2, 3)

    for h in range(heads):
        at = slice(h * 256, (h + 1) * 256)
        att[:, h * HEAD : (h + 1) * HEAD] = (
            (acc[0:HEAD, at] / acc[HEAD : HEAD + 1, at]).T
        ).astype(BF)

    wcopies[3].wait()
    piece = BLK // 2
    mine = pl.ds(pl.multiple_of(core * piece, piece), piece)
    other = pl.ds(pl.multiple_of((1 - core) * piece, piece), piece)
    far_rows = pl.ds(pl.multiple_of((1 - zhi) * BLK, BLK), BLK)
    near_rows = pl.ds(pl.multiple_of(zhi * BLK, BLK), BLK)
    order = (0, 2, 1, 3)
    far_mate = [copy_to(d_out.at[j], d_in.at[j], mate) for j in range(4)]
    near_mate = [copy_to(dl_out.at[j], dl_in.at[j], mate) for j in range(4)]
    first_hop = [
        copy_to(zs_out.at[j], zr_rel.at[j], up if j < 2 else down) for j in range(4)
    ]
    second_hop = [
        copy_to(zr_rel.at[j], zr_in.at[j], up if j < 2 else down) for j in range(4)
    ]

    def pass_on(j):
        far_mate[j].wait_recv()
        zs_out[j] = (prem[j, mine, :] + d_in[j].astype(F32)).astype(BF)
        first_hop[j].start()

    last = None
    for j in order:
        prem[j] = dot(att[far_rows, :], wo[:, j * d : (j + 1) * d])
        d_out[j] = prem[j, other, :].astype(BF)
        far_mate[j].start()
        if last is not None:
            pass_on(last)
        last = j
    pass_on(last)
    for k, j in enumerate(order):
        ploc[j] = dot(att[near_rows, :], wo[:, j * d : (j + 1) * d])
        dl_out[j] = ploc[j, other, :].astype(BF)
        near_mate[j].start()
    for j in order:
        first_hop[j].wait_recv()
        second_hop[j].start()
    for j in order:
        near_mate[j].wait_recv()
        ploc[j, mine, :] += dl_in[j].astype(F32)

    gate = 1.0 / (1.0 + jnp.exp(-gsum[zhi, mine, 0:1]))
    for j in order:
        second_hop[j].wait_recv()
    for ref, s in ((own, src_own), (part, src_mate), (zsame, src_same), (zother, src_other)):
        total = ploc[s, mine, :] + zr_in[s].astype(F32)
        out[:, pl.ds(pl.multiple_of(s * d, d), d)] = (ref[zhi, mine, :].astype(F32) + gate * total).astype(BF)

    for copy in made:
        copy.wait_send()


def on_device(resid, sel_blocks, norm_gain, router_weight, w_query, w_key, value_projection, w_out):
    local_rows, d = resid.shape
    width = w_out.shape[1]
    count = local_rows // BLK
    freqs = jnp.exp(
        jnp.arange(HEAD // 2, dtype=F32) * (-2.0 * math.log(rope_base) / HEAD)
    )
    freqs = jnp.concatenate([freqs, freqs]).reshape(1, HEAD)
    qcols = w_query.shape[1]
    heads = qcols // HEAD
    vmem = pl.BlockSpec(memory_space=pltpu.VMEM)
    anyspace = pl.BlockSpec(memory_space=pl.ANY)
    piece = BLK // 2
    nsem = 74
    result = pl.pallas_call(
        layer_kernel,
        name="layer",
        out_shape=jax.ShapeDtypeStruct((piece, width), BF),
        in_specs=[pl.BlockSpec(memory_space=pltpu.SMEM)] + [vmem] * 3 + [anyspace] * 5,
        out_specs=vmem,
        scratch_shapes=[
            pltpu.VMEM((count, BLK, d), BF),
            pltpu.VMEM((2, BLK, d), BF),
            pltpu.VMEM((2, BLK, HEAD), F32),
            pltpu.VMEM((2, BLK, HEAD), F32),
            pltpu.VMEM((width, qcols), BF),
            pltpu.VMEM((width, 2 * HEAD), BF),
            pltpu.VMEM((qcols, width), BF),
            pltpu.VMEM((2, BLK, d), BF),
            pltpu.VMEM((2, BLK, d), BF),
            pltpu.VMEM((2, BLK, d), BF),
            pltpu.VMEM((2, BLK, d // 2), BF),
            pltpu.VMEM((2, BLK, d // 2), BF),
            pltpu.VMEM((2, BLK, qcols), F32),
            pltpu.VMEM((2, BLK, 2 * HEAD), F32),
            pltpu.VMEM((2, BLK, HEAD), F32),
            pltpu.VMEM((2, BLK, HEAD), F32),
            pltpu.VMEM((heads * 256, HEAD), BF),
            pltpu.VMEM((8, 8 * BLK, 2 * HEAD), BF),
            pltpu.VMEM((8, heads * 256), F32),
            pltpu.VMEM((HEAD + 16, heads * 256), F32),
            pltpu.VMEM((2, 8 * BLK, 512), F32),
            pltpu.VMEM((2, 8 * BLK, 512), BF),
            pltpu.VMEM((2, 8, 512), F32),
            pltpu.VMEM((256, qcols), BF),
            pltpu.VMEM((4, BLK, d), F32),
            pltpu.VMEM((4, BLK, d), F32),
            pltpu.VMEM((4, piece, d), BF),
            pltpu.VMEM((4, piece, d), BF),
            pltpu.VMEM((4, piece, d), BF),
            pltpu.VMEM((4, piece, d), BF),
            pltpu.VMEM((4, piece, d), BF),
            pltpu.VMEM((4, piece, d), BF),
            pltpu.VMEM((4, piece, d), BF),
            pltpu.SemaphoreType.DMA((nsem,)),
            pltpu.SemaphoreType.DMA((nsem,)),
            pltpu.SemaphoreType.DMA((5,)),
        ],
        compiler_params=pltpu.CompilerParams(
            collective_id=0, has_side_effects=True, vmem_limit_bytes=60 * 1024 * 1024
        ),
    )(
        sel_blocks, freqs, norm_gain.reshape(1, width), router_weight.reshape(1, width),
        resid.reshape(count, BLK, d), w_query, w_key, value_projection, w_out,
    )
    return result


def solution(mesh):
    return jax.shard_map(
        on_device,
        mesh=mesh,
        in_specs=(
            P("ctx", "tp"),
            P("ctx"),
            P(),
            P(),
            P(None, "tp"),
            P(None, "tp"),
            P(None, "tp"),
            P("tp", None),
        ),
        out_specs=P(("ctx", "tp"), None),
        check_vma=False,
    )
```

```python
import math

import jax
import jax.numpy as jnp
from jax import lax
from jax.experimental import pallas as pl
from jax.experimental.pallas import tpu as pltpu
from jax.sharding import PartitionSpec as P

HEAD = 128
BLK = 128
MESH = pl.DeviceIdType.MESH
BF = jnp.bfloat16
F32 = jnp.float32

rope_base = 500000.0
norm_eps = 1e-05
LOW = -1e30


def dot(a, b):
    return jnp.dot(a, b, preferred_element_type=F32)


def layer_kernel(
    sel, freq, gain, router, resid_hbm, wq_hbm, wk_hbm, wv_hbm, wo_hbm,
    out,
    resid, own, cosf, sinf, wq, wkv, wo, part, zsame, zother, rel_p, rel_m,
    qacc, kvacc, ssq, gsum, q, buf, m_ref, acc, s_ref, p_ref, x_ref, att,
    prem, ploc, d_out, d_in, dl_out, dl_in, zs_out, zr_rel, zr_in,
    ssem, rsem, wsem,
):
    c = lax.axis_index("ctx")
    t = lax.axis_index("tp")
    x, zlo, y = c // 8, (c // 4) % 2, c % 4
    zhi, core = t // 2, t % 2
    z = zhi * 2 + zlo
    d = own.shape[2]
    half = d // 2
    heads = q.shape[0] // 256
    width = wo.shape[1]
    nchunk = width // d

    def dev(dx=0, dy=0, dz=0, dc=0):
        nx, ny, nz = (x + dx + 4) % 4, (y + dy + 4) % 4, (z + dz + 4) % 4
        return (nx * 8 + (nz % 2) * 4 + ny, (nz // 2) * 2 + (core + dc) % 2)

    right_x, left_x = dev(dx=1), dev(dx=-1)
    right_y, left_y = dev(dy=1), dev(dy=-1)
    up, down = dev(dz=1), dev(dz=-1)
    mate = dev(dc=1)
    zpair = (x * 8 + (1 - zlo) * 4 + y, t)

    wcopies = [
        pltpu.make_async_copy(wq_hbm, wq, wsem.at[0]),
        pltpu.make_async_copy(wk_hbm, wkv.at[:, 0:HEAD], wsem.at[1]),
        pltpu.make_async_copy(wv_hbm, wkv.at[:, HEAD : 2 * HEAD], wsem.at[2]),
        pltpu.make_async_copy(wo_hbm, wo, wsem.at[3]),
    ]
    rcopy = pltpu.make_async_copy(resid_hbm, resid, wsem.at[4])
    rcopy.start()
    for copy in wcopies:
        copy.start()

    barrier = pltpu.get_barrier_semaphore()
    for peer in (mate, up, down, right_x, left_x, right_y, left_y):
        pl.semaphore_signal(barrier, inc=1, device_id=peer, device_id_type=MESH)
    rcopy.wait()
    for b in range(2):
        at = jnp.clip(sel[b] - c * resid.shape[0], 0, resid.shape[0] - 1)
        own[b] = resid[at]
    pl.semaphore_wait(barrier, 7)

    made = []

    def copy_to(src, dst, peer):
        k = len(made)
        copy = pltpu.make_async_remote_copy(
            src_ref=src, dst_ref=dst, send_sem=ssem.at[k], recv_sem=rsem.at[k],
            device_id=peer, device_id_type=MESH,
        )
        made.append(copy)
        return copy

    to_mate = [copy_to(own.at[b], part.at[b], mate) for b in range(2)]
    to_up = [copy_to(own.at[b, :, 0:half], rel_p.at[b], up) for b in range(2)]
    to_down = [copy_to(own.at[b, :, half:d], rel_m.at[b], down) for b in range(2)]
    fwd_up = [copy_to(rel_p.at[b], zsame.at[b, :, 0:half], up) for b in range(2)]
    fwd_down = [copy_to(rel_m.at[b], zsame.at[b, :, half:d], down) for b in range(2)]
    fwd_mate = [copy_to(zsame.at[b], zother.at[b], mate) for b in range(2)]
    for b in range(2):
        to_up[b].start()
        to_down[b].start()
        to_mate[b].start()

    lane = lax.broadcasted_iota(jnp.int32, (BLK, HEAD), 1)
    row = lax.broadcasted_iota(jnp.int32, (BLK, HEAD), 0)
    for b in range(2):
        angle = (row + sel[b] * BLK).astype(F32) * freq[...]
        cosf[b] = jnp.cos(angle)
        sine = jnp.sin(angle)
        sinf[b] = jnp.where(lane < HEAD // 2, -sine, sine)
    ssq[...] = jnp.zeros_like(ssq)
    gsum[...] = jnp.zeros_like(gsum)
    src_own, src_mate = t, t + 1 - 2 * core
    src_same = (t + 2) % 4
    src_other = (src_mate + 2) % 4

    def project(ref, b, s, first):
        at = pl.multiple_of(s * d, d)
        rows = pl.ds(at, d)
        ch = ref[b].astype(F32)
        ssq[b] += jnp.broadcast_to(jnp.sum(ch * ch, axis=1, keepdims=True), (BLK, HEAD))
        gsum[b] += jnp.broadcast_to(
            jnp.sum(ch * router[:, rows], axis=1, keepdims=True), (BLK, HEAD)
        )
        cg = (ch * gain[:, rows]).astype(BF)
        pq = dot(cg, wq[rows, :])
        pkv = dot(cg, wkv[rows, :])
        if first:
            qacc[b] = pq
            kvacc[b] = pkv
        else:
            qacc[b] += pq
            kvacc[b] += pkv

    for copy in wcopies[:3]:
        copy.wait()
    for b in range(2):
        project(own, b, src_own, True)
    for b in range(2):
        to_up[b].wait_recv()
        fwd_up[b].start()
        to_down[b].wait_recv()
        fwd_down[b].start()
        if b == 0:
            for bb in range(2):
                to_mate[bb].wait_recv()
                project(part, bb, src_mate, False)
    for b in range(2):
        fwd_up[b].wait_recv()
        fwd_down[b].wait_recv()
        fwd_mate[b].start()
        project(zsame, b, src_same, False)
    for b in range(2):
        fwd_mate[b].wait_recv()
        project(zother, b, src_other, False)

    def rotated(v, b):
        return v * cosf[b] + pltpu.roll(v, HEAD // 2, 1) * sinf[b]

    def unit_at(base, i, j, k):
        return buf.at[base + i, pl.ds(pl.multiple_of((j * 2 + k) * BLK, BLK), BLK)]

    own_a = unit_at(0, y, x, zlo)
    own_b = unit_at(4, x, y, zlo)
    scale = math.log2(math.e) / math.sqrt(HEAD)
    for b, unit in ((0, own_a), (1, own_b)):
        inv = lax.rsqrt(ssq[b][:, 0:1] * (1.0 / width) + norm_eps)
        kv = kvacc[b] * inv
        unit[:, 0:HEAD] = rotated(kv[:, 0:HEAD], b).astype(BF)
        unit[:, HEAD : 2 * HEAD] = kv[:, HEAD:].T.astype(BF)

    class Side:
        def __init__(self, base, i, j, plus1, minus1, plus2, minus2):
            self.base, self.i, self.j = base, i, j
            first, second = (plus1, minus1), (plus2, minus2)
            self.to_z = self.send(0, 0, 0, zpair)
            self.own1 = [self.send(0, 0, 0, peer) for peer in first]
            self.own2 = [self.send(0, 0, 0, peer) for peer in second]
            self.z1 = [self.send(0, 0, 1, peer) for peer in first]
            self.z2 = [self.send(0, 0, 1, peer) for peer in second]
            self.half1 = [self.send(0, -1, 0, plus1), self.send(0, 1, 1, minus1)]
            self.cross = {
                (r, k): [self.send(0, r, k, peer) for peer in second]
                for r in (-1, 1, 2)
                for k in range(2)
            }
            self.far = {
                (r, k): self.send(1 if k else -1, r, k, minus2 if k else plus2)
                for r in (0, -1, 1, 2)
                for k in range(2)
            }

        def place(self, di, dj, k):
            plane = 1 - zlo if k else zlo
            return lax.rem(self.i + di + 4, 4), lax.rem(self.j + dj + 4, 4), plane

        def unit(self, di, dj, k):
            return unit_at(self.base, *self.place(di, dj, k))

        def send(self, di, dj, k, peer):
            return copy_to(self.unit(di, dj, k), self.unit(di, dj, k), peer)

        def allowed(self, di, dj, k):
            i, j, plane = self.place(di, dj, k)
            return (i * 8 + j if self.base else j * 8 + i) + plane * 4 < c

    sides = (
        Side(0, y, x, right_x, left_x, right_y, left_y),
        Side(4, x, y, right_y, left_y, right_x, left_x),
    )

    def start(*groups):
        for group in groups:
            for copy in group:
                copy.start()

    for s in sides:
        s.to_z.start()
        start(s.own1, s.own2)

    for b in range(2):
        inv = lax.rsqrt(ssq[b][:, 0:1] * (1.0 / width) + norm_eps)
        for h in range(heads):
            qh = qacc[b][:, h * HEAD : (h + 1) * HEAD] * inv
            q[h * 256 + b * BLK : h * 256 + (b + 1) * BLK, :] = (
                rotated(qh, b) * scale
            ).astype(BF)

    cols = 512
    tiles = heads * 256 // cols
    ones_rows = jnp.ones((16, 8 * BLK), BF)

    def scores_of(ks, r):
        return lax.dot_general(
            ks, q[r * cols : (r + 1) * cols, :], (((1,), (1,)), ((), ())),
            preferred_element_type=F32,
        )

    keys_own = jnp.concatenate([own_a[:, 0:HEAD], own_b[:, 0:HEAD]], axis=0)
    v_own = jnp.concatenate([own_a[:, HEAD:], own_b[:, HEAD:]], axis=1)
    v_own = jnp.concatenate([v_own, ones_rows[:, 0 : 2 * BLK]], axis=0)
    key_at = lax.broadcasted_iota(jnp.int32, (256, cols), 0)
    query_at = lax.broadcasted_iota(jnp.int32, (256, cols), 1) & 255
    upper = key_at <= query_at
    for r in range(tiles):
        at = slice(r * cols, (r + 1) * cols)
        sc = jnp.where(upper, scores_of(keys_own, r), LOW)
        high = jnp.max(sc, axis=0, keepdims=True)
        pr = jnp.where(upper, jnp.exp2(sc - high), 0.0).astype(BF)
        m_ref[:, at] = jnp.broadcast_to(high, (8, cols))
        acc[:, at] = dot(v_own, pr)

    def attend(places):
        units = [(s, p) for s in sides for p in places]
        allowed = [s.allowed(*p) for s, p in units]
        some = allowed[0]
        for flag in allowed[1:]:
            some = jnp.logical_or(some, flag)

        @pl.when(some)
        def _():
            def score(r):
                ks = jnp.concatenate([s.unit(*p)[:, 0:HEAD] for s, p in units], axis=0)
                sc = scores_of(ks, r)
                s_ref[r % 2] = jnp.concatenate(
                    [
                        sc[u * BLK : (u + 1) * BLK] + jnp.where(allowed[u], 0.0, LOW)
                        for u in range(8)
                    ],
                    axis=0,
                )

            def soften(r):
                at = slice(r * cols, (r + 1) * cols)
                sc = s_ref[r % 2]
                old = m_ref[0:1, at]
                high = jnp.maximum(old, jnp.max(sc, axis=0, keepdims=True))
                p_ref[r % 2] = jnp.exp2(sc - high).astype(BF)
                x_ref[r % 2] = jnp.broadcast_to(jnp.exp2(old - high), (8, cols))
                m_ref[:, at] = jnp.broadcast_to(high, (8, cols))

            def collect(r):
                at = slice(r * cols, (r + 1) * cols)
                vt = jnp.concatenate(
                    [s.unit(*p)[:, HEAD:] for s, p in units], axis=1
                )
                vt = jnp.concatenate([vt, ones_rows], axis=0)
                acc[:, at] = acc[:, at] * x_ref[r % 2][0:1] + dot(vt, p_ref[r % 2])

            for k in range(tiles + 2):
                if k < tiles:
                    score(k)
                if k >= 2:
                    collect(k - 2)
                if 1 <= k <= tiles:
                    soften(k - 1)

    for s in sides:
        s.to_z.wait_recv()
        start(s.z1, s.z2)
    for s in sides:
        s.own1[0].wait_recv()
        s.half1[0].start()
        start(s.cross[-1, 0])
        s.own1[1].wait_recv()
        start(s.cross[1, 0])
        s.own2[0].wait_recv()
        s.far[0, 0].start()
        s.own2[1].wait_recv()
    attend([(0, -1, 0), (0, 1, 0), (-1, 0, 0), (1, 0, 0)])
    for s in sides:
        s.z1[0].wait_recv()
        start(s.cross[-1, 1])
        s.z1[1].wait_recv()
        s.half1[1].start()
        start(s.cross[1, 1])
        s.z2[0].wait_recv()
        s.z2[1].wait_recv()
        s.far[0, 1].start()
    attend([(0, -1, 1), (0, 1, 1), (-1, 0, 1), (1, 0, 1)])

    def relay(r, k):
        for s in sides:
            for copy in s.cross[r, k]:
                copy.wait_recv()
            s.far[r, k].start()

    for s in sides:
        s.half1[0].wait_recv()
        start(s.cross[2, 0])
    relay(-1, 0)
    relay(1, 0)
    attend([(di, dj, 0) for di in (-1, 1) for dj in (-1, 1)])
    for s in sides:
        s.half1[1].wait_recv()
        start(s.cross[2, 1])
    attend([(0, 0, 0), (0, 0, 1), (0, 2, 0), (0, 2, 1)])
    relay(-1, 1)
    relay(1, 1)
    attend([(di, dj, 1) for di in (-1, 1) for dj in (-1, 1)])
    relay(2, 0)
    relay(2, 1)
    attend([(di, 2, k) for di in (-1, 1) for k in range(2)])
    for rs in ((0, -1), (1, 2)):
        for s in sides:
            for r in rs:
                s.far[r, 0].wait_recv()
                s.far[r, 1].wait_recv()
        attend([(2, r, k) for r in rs for k in range(2)])

    for h in range(heads):
        at = slice(h * 256, (h + 1) * 256)
        att[:, h * HEAD : (h + 1) * HEAD] = (
            (acc[0:HEAD, at] / acc[HEAD : HEAD + 1, at]).T
        ).astype(BF)

    wcopies[3].wait()
    piece = BLK // 2
    mine = pl.ds(pl.multiple_of(core * piece, piece), piece)
    other = pl.ds(pl.multiple_of((1 - core) * piece, piece), piece)
    far_rows = pl.ds(pl.multiple_of((1 - zhi) * BLK, BLK), BLK)
    near_rows = pl.ds(pl.multiple_of(zhi * BLK, BLK), BLK)
    order = (0, 2, 1, 3)
    far_mate = [copy_to(d_out.at[j], d_in.at[j], mate) for j in range(4)]
    near_mate = [copy_to(dl_out.at[j], dl_in.at[j], mate) for j in range(4)]
    first_hop = [
        copy_to(zs_out.at[j], zr_rel.at[j], up if j < 2 else down) for j in range(4)
    ]
    second_hop = [
        copy_to(zr_rel.at[j], zr_in.at[j], up if j < 2 else down) for j in range(4)
    ]

    def pass_on(j):
        far_mate[j].wait_recv()
        zs_out[j] = (prem[j, mine, :] + d_in[j].astype(F32)).astype(BF)
        first_hop[j].start()

    last = None
    for j in order:
        prem[j] = dot(att[far_rows, :], wo[:, j * d : (j + 1) * d])
        d_out[j] = prem[j, other, :].astype(BF)
        far_mate[j].start()
        if last is not None:
            pass_on(last)
        last = j
    pass_on(last)
    for k, j in enumerate(order):
        ploc[j] = dot(att[near_rows, :], wo[:, j * d : (j + 1) * d])
        dl_out[j] = ploc[j, other, :].astype(BF)
        near_mate[j].start()
    for j in order:
        first_hop[j].wait_recv()
        second_hop[j].start()
    for j in order:
        near_mate[j].wait_recv()
        ploc[j, mine, :] += dl_in[j].astype(F32)

    gate = 1.0 / (1.0 + jnp.exp(-gsum[zhi, mine, 0:1]))
    for j in order:
        second_hop[j].wait_recv()
    for ref, s in ((own, src_own), (part, src_mate), (zsame, src_same), (zother, src_other)):
        total = ploc[s, mine, :] + zr_in[s].astype(F32)
        out[:, pl.ds(pl.multiple_of(s * d, d), d)] = (ref[zhi, mine, :].astype(F32) + gate * total).astype(BF)

    for copy in made:
        copy.wait_send()


def on_device(resid, sel_blocks, norm_gain, router_weight, w_query, w_key, value_projection, w_out):
    local_rows, d = resid.shape
    width = w_out.shape[1]
    count = local_rows // BLK
    freqs = jnp.exp(
        jnp.arange(HEAD // 2, dtype=F32) * (-2.0 * math.log(rope_base) / HEAD)
    )
    freqs = jnp.concatenate([freqs, freqs]).reshape(1, HEAD)
    qcols = w_query.shape[1]
    heads = qcols // HEAD
    vmem = pl.BlockSpec(memory_space=pltpu.VMEM)
    anyspace = pl.BlockSpec(memory_space=pl.ANY)
    piece = BLK // 2
    nsem = 90
    result = pl.pallas_call(
        layer_kernel,
        name="layer",
        out_shape=jax.ShapeDtypeStruct((piece, width), BF),
        in_specs=[pl.BlockSpec(memory_space=pltpu.SMEM)] + [vmem] * 3 + [anyspace] * 5,
        out_specs=vmem,
        scratch_shapes=[
            pltpu.VMEM((count, BLK, d), BF),
            pltpu.VMEM((2, BLK, d), BF),
            pltpu.VMEM((2, BLK, HEAD), F32),
            pltpu.VMEM((2, BLK, HEAD), F32),
            pltpu.VMEM((width, qcols), BF),
            pltpu.VMEM((width, 2 * HEAD), BF),
            pltpu.VMEM((qcols, width), BF),
            pltpu.VMEM((2, BLK, d), BF),
            pltpu.VMEM((2, BLK, d), BF),
            pltpu.VMEM((2, BLK, d), BF),
            pltpu.VMEM((2, BLK, d // 2), BF),
            pltpu.VMEM((2, BLK, d // 2), BF),
            pltpu.VMEM((2, BLK, qcols), F32),
            pltpu.VMEM((2, BLK, 2 * HEAD), F32),
            pltpu.VMEM((2, BLK, HEAD), F32),
            pltpu.VMEM((2, BLK, HEAD), F32),
            pltpu.VMEM((heads * 256, HEAD), BF),
            pltpu.VMEM((8, 8 * BLK, 2 * HEAD), BF),
            pltpu.VMEM((8, heads * 256), F32),
            pltpu.VMEM((HEAD + 16, heads * 256), F32),
            pltpu.VMEM((2, 8 * BLK, 512), F32),
            pltpu.VMEM((2, 8 * BLK, 512), BF),
            pltpu.VMEM((2, 8, 512), F32),
            pltpu.VMEM((256, qcols), BF),
            pltpu.VMEM((4, BLK, d), F32),
            pltpu.VMEM((4, BLK, d), F32),
            pltpu.VMEM((4, piece, d), BF),
            pltpu.VMEM((4, piece, d), BF),
            pltpu.VMEM((4, piece, d), BF),
            pltpu.VMEM((4, piece, d), BF),
            pltpu.VMEM((4, piece, d), BF),
            pltpu.VMEM((4, piece, d), BF),
            pltpu.VMEM((4, piece, d), BF),
            pltpu.SemaphoreType.DMA((nsem,)),
            pltpu.SemaphoreType.DMA((nsem,)),
            pltpu.SemaphoreType.DMA((5,)),
        ],
        compiler_params=pltpu.CompilerParams(
            collective_id=0, has_side_effects=True, vmem_limit_bytes=60 * 1024 * 1024
        ),
    )(
        sel_blocks, freqs, norm_gain.reshape(1, width), router_weight.reshape(1, width),
        resid.reshape(count, BLK, d), w_query, w_key, value_projection, w_out,
    )
    return result


def solution(mesh):
    return jax.shard_map(
        on_device,
        mesh=mesh,
        in_specs=(
            P("ctx", "tp"),
            P("ctx"),
            P(),
            P(),
            P(None, "tp"),
            P(None, "tp"),
            P(None, "tp"),
            P("tp", None),
        ),
        out_specs=P(("ctx", "tp"), None),
        check_vma=False,
    )
```

```python
import math

import jax
import jax.numpy as jnp
from jax import lax
from jax.experimental import pallas as pl
from jax.experimental.pallas import tpu as pltpu
from jax.sharding import PartitionSpec as P

HEAD = 128
BLK = 128
MESH = pl.DeviceIdType.MESH
BF = jnp.bfloat16
F32 = jnp.float32

rope_base = 500000.0
norm_eps = 1e-05
LOW = -1e30


def dot(a, b):
    return jnp.dot(a, b, preferred_element_type=F32)


def layer_kernel(
    sel, freq, gain, router, resid_hbm, wq_hbm, wk_hbm, wv_hbm, wo_hbm,
    out,
    resid, own, cosf, sinf, wq, wkv, wo, part, zsame, zother, rel_p, rel_m,
    qacc, kvacc, ssq, gsum, q, buf, m_ref, acc, s_ref, p_ref, x_ref, att,
    prem, ploc, d_out, d_in, dl_out, dl_in, zs_out, zr_rel, zr_in,
    ssem, rsem, wsem,
):
    c = lax.axis_index("ctx")
    t = lax.axis_index("tp")
    x, zlo, y = c // 8, (c // 4) % 2, c % 4
    zhi, core = t // 2, t % 2
    z = zhi * 2 + zlo
    d = own.shape[2]
    half = d // 2
    heads = q.shape[0] // 256
    width = wo.shape[1]
    nchunk = width // d

    def dev(dx=0, dy=0, dz=0, dc=0):
        nx, ny, nz = (x + dx + 4) % 4, (y + dy + 4) % 4, (z + dz + 4) % 4
        return (nx * 8 + (nz % 2) * 4 + ny, (nz // 2) * 2 + (core + dc) % 2)

    right_x, left_x = dev(dx=1), dev(dx=-1)
    right_y, left_y = dev(dy=1), dev(dy=-1)
    up, down = dev(dz=1), dev(dz=-1)
    mate = dev(dc=1)
    zpair = (x * 8 + (1 - zlo) * 4 + y, t)

    wcopies = [
        pltpu.make_async_copy(wq_hbm, wq, wsem.at[0]),
        pltpu.make_async_copy(wk_hbm, wkv.at[:, 0:HEAD], wsem.at[1]),
        pltpu.make_async_copy(wv_hbm, wkv.at[:, HEAD : 2 * HEAD], wsem.at[2]),
        pltpu.make_async_copy(wo_hbm, wo, wsem.at[3]),
    ]
    rcopy = pltpu.make_async_copy(resid_hbm, resid, wsem.at[4])
    rcopy.start()
    for copy in wcopies:
        copy.start()

    barrier = pltpu.get_barrier_semaphore()
    for peer in (mate, up, down, right_x, left_x, right_y, left_y):
        pl.semaphore_signal(barrier, inc=1, device_id=peer, device_id_type=MESH)
    rcopy.wait()
    for b in range(2):
        at = jnp.clip(sel[b] - c * resid.shape[0], 0, resid.shape[0] - 1)
        own[b] = resid[at]
    pl.semaphore_wait(barrier, 7)

    made = []

    def copy_to(src, dst, peer):
        k = len(made)
        copy = pltpu.make_async_remote_copy(
            src_ref=src, dst_ref=dst, send_sem=ssem.at[k], recv_sem=rsem.at[k],
            device_id=peer, device_id_type=MESH,
        )
        made.append(copy)
        return copy

    to_mate = [copy_to(own.at[b], part.at[b], mate) for b in range(2)]
    to_up = [copy_to(own.at[b, :, 0:half], rel_p.at[b], up) for b in range(2)]
    to_down = [copy_to(own.at[b, :, half:d], rel_m.at[b], down) for b in range(2)]
    fwd_up = [copy_to(rel_p.at[b], zsame.at[b, :, 0:half], up) for b in range(2)]
    fwd_down = [copy_to(rel_m.at[b], zsame.at[b, :, half:d], down) for b in range(2)]
    fwd_mate = [copy_to(zsame.at[b], zother.at[b], mate) for b in range(2)]
    for b in range(2):
        to_up[b].start()
        to_down[b].start()
        to_mate[b].start()

    def rotated(v, b):
        return v * cosf[b] + pltpu.roll(v, HEAD // 2, 1) * sinf[b]

    def unit_at(base, i, j, k):
        return buf.at[base + i, pl.ds(pl.multiple_of((j * 2 + k) * BLK, BLK), BLK)]

    own_a = unit_at(0, y, x, zlo)
    own_b = unit_at(4, x, y, zlo)
    scale = math.log2(math.e) / math.sqrt(HEAD)
    span = heads * BLK

    def finish_keys(b):
        unit = own_b if b else own_a
        kv = kvacc[b] * lax.rsqrt(ssq[b][:, 0:1] * (1.0 / width) + norm_eps)
        unit[:, 0:HEAD] = rotated(kv[:, 0:HEAD], b).astype(BF)
        unit[:, HEAD : 2 * HEAD] = kv[:, HEAD:].T.astype(BF)

    def finish_queries(b):
        inv = lax.rsqrt(ssq[b][:, 0:1] * (1.0 / width) + norm_eps)
        for h in range(heads):
            qh = qacc[b][:, h * HEAD : (h + 1) * HEAD] * inv
            at = b * span + h * BLK
            q[at : at + BLK, :] = (rotated(qh, b) * scale).astype(BF)

    class Side:
        def __init__(self, base, i, j, plus1, minus1, plus2, minus2):
            self.base, self.i, self.j = base, i, j
            first, second = (plus1, minus1), (plus2, minus2)
            self.to_z = self.send(0, 0, 0, zpair)
            self.own1 = [self.send(0, 0, 0, peer) for peer in first]
            self.own2 = [self.send(0, 0, 0, peer) for peer in second]
            self.z1 = [self.send(0, 0, 1, peer) for peer in first]
            self.z2 = [self.send(0, 0, 1, peer) for peer in second]
            self.half1 = [self.send(0, -1, 0, plus1), self.send(0, 1, 1, minus1)]
            self.cross = {
                (r, k): [self.send(0, r, k, peer) for peer in second]
                for r in (-1, 1, 2)
                for k in range(2)
            }
            self.far = {
                (r, k): self.send(1 if k else -1, r, k, minus2 if k else plus2)
                for r in (0, -1, 1, 2)
                for k in range(2)
            }

        def place(self, di, dj, k):
            plane = 1 - zlo if k else zlo
            return lax.rem(self.i + di + 4, 4), lax.rem(self.j + dj + 4, 4), plane

        def unit(self, di, dj, k):
            return unit_at(self.base, *self.place(di, dj, k))

        def send(self, di, dj, k, peer):
            return copy_to(self.unit(di, dj, k), self.unit(di, dj, k), peer)

        def allowed(self, di, dj, k):
            i, j, plane = self.place(di, dj, k)
            return (i * 8 + j if self.base else j * 8 + i) + plane * 4 < c

    sides = (
        Side(0, y, x, right_x, left_x, right_y, left_y),
        Side(4, x, y, right_y, left_y, right_x, left_x),
    )

    def start(*groups):
        for group in groups:
            for copy in group:
                copy.start()

    lane = lax.broadcasted_iota(jnp.int32, (BLK, HEAD), 1)
    row = lax.broadcasted_iota(jnp.int32, (BLK, HEAD), 0)
    for b in range(2):
        angle = (row + sel[b] * BLK).astype(F32) * freq[...]
        cosf[b] = jnp.cos(angle)
        sine = jnp.sin(angle)
        sinf[b] = jnp.where(lane < HEAD // 2, -sine, sine)
    ssq[...] = jnp.zeros_like(ssq)
    gsum[...] = jnp.zeros_like(gsum)
    src_own, src_mate = t, t + 1 - 2 * core
    src_same = (t + 2) % 4
    src_other = (src_mate + 2) % 4

    def project(ref, b, s, first=False):
        rows = pl.ds(pl.multiple_of(s * d, d), d)
        ch = ref[b].astype(F32)
        ssq[b] += jnp.broadcast_to(jnp.sum(ch * ch, axis=1, keepdims=True), (BLK, HEAD))
        gsum[b] += jnp.broadcast_to(
            jnp.sum(ch * router[:, rows], axis=1, keepdims=True), (BLK, HEAD)
        )
        cg = (ch * gain[:, rows]).astype(BF)

        def into(total, weight):
            part_sum = dot(cg, weight[rows, :])
            if first:
                total[b] = part_sum
            else:
                total[b] += part_sum

        into(kvacc, wkv)
        return lambda: into(qacc, wq)

    def relay_features(b):
        to_up[b].wait_recv()
        fwd_up[b].start()
        to_down[b].wait_recv()
        fwd_down[b].start()

    relay_features(0)
    for copy in wcopies[:3]:
        copy.wait()
    for b in range(2):
        project(own, b, src_own, True)()
    relay_features(1)
    for b in range(2):
        to_mate[b].wait_recv()
        project(part, b, src_mate)()
    for b in range(2):
        fwd_up[b].wait_recv()
        fwd_down[b].wait_recv()
        fwd_mate[b].start()
        project(zsame, b, src_same)()
        fwd_mate[b].wait_recv()
        rest = project(zother, b, src_other)
        finish_keys(b)
        sides[b].to_z.start()
        start(sides[b].own1, sides[b].own2)
        rest()
        finish_queries(b)

    cols = 512
    tiles = span // cols
    ones_rows = jnp.ones((16, 8 * BLK), BF)

    def scores_of(ks, at):
        return lax.dot_general(
            ks, q[at, :], (((1,), (1,)), ((), ())), preferred_element_type=F32
        )

    keys_own = jnp.concatenate([own_a[:, 0:HEAD], own_b[:, 0:HEAD]], axis=0)
    v_own = jnp.concatenate([own_a[:, HEAD:], own_b[:, HEAD:]], axis=1)
    v_own = jnp.concatenate([v_own, ones_rows[:, 0 : 2 * BLK]], axis=0)
    key_at = lax.broadcasted_iota(jnp.int32, (256, cols), 0)
    query_at = lax.broadcasted_iota(jnp.int32, (256, cols), 1) & (BLK - 1)
    for r in range(2 * tiles):
        at = slice(r * cols, (r + 1) * cols)
        seen = key_at <= query_at + (r // tiles) * BLK
        sc = jnp.where(seen, scores_of(keys_own, at), LOW)
        high = jnp.max(sc, axis=0, keepdims=True)
        pr = jnp.where(seen, jnp.exp2(sc - high), 0.0).astype(BF)
        m_ref[:, at] = jnp.broadcast_to(high, (8, cols))
        acc[:, at] = dot(v_own, pr)

    def attend(groups, block=None):
        units = [[(s, p) for s in sides for p in places] for places in groups]
        allowed = [[s.allowed(*p) for s, p in group] for group in units]
        some = allowed[0][0]
        for flags in allowed:
            for flag in flags:
                some = jnp.logical_or(some, flag)
        if block is None:
            spots = [slice(r * cols, (r + 1) * cols) for r in range(2 * tiles)]
        else:
            spots = [
                pl.ds(pl.multiple_of(block * span + r * cols, cols), cols)
                for r in range(tiles)
            ]
        steps = [(g, at) for g in range(len(groups)) for at in spots]

        @pl.when(some)
        def _():
            def score(k):
                g, at = steps[k]
                ks = jnp.concatenate([s.unit(*p)[:, 0:HEAD] for s, p in units[g]], axis=0)
                sc = scores_of(ks, at)
                s_ref[k % 2] = jnp.concatenate(
                    [
                        sc[u * BLK : (u + 1) * BLK] + jnp.where(allowed[g][u], 0.0, LOW)
                        for u in range(8)
                    ],
                    axis=0,
                )

            def soften(k):
                at = steps[k][1]
                sc = s_ref[k % 2]
                old = m_ref[0:1, at]
                high = jnp.maximum(old, jnp.max(sc, axis=0, keepdims=True))
                p_ref[k % 2] = jnp.exp2(sc - high).astype(BF)
                x_ref[k % 2] = jnp.broadcast_to(jnp.exp2(old - high), (8, cols))
                m_ref[:, at] = jnp.broadcast_to(high, (8, cols))

            def collect(k):
                g, at = steps[k]
                vt = jnp.concatenate([s.unit(*p)[:, HEAD:] for s, p in units[g]], axis=1)
                vt = jnp.concatenate([vt, ones_rows], axis=0)
                acc[:, at] = acc[:, at] * x_ref[k % 2][0:1] + dot(vt, p_ref[k % 2])

            count = len(steps)
            for k in range(count + 2):
                if k < count:
                    score(k)
                if k >= 2:
                    collect(k - 2)
                if 1 <= k <= count:
                    soften(k - 1)

    for s in sides:
        s.to_z.wait_recv()
        start(s.z1, s.z2)
    for s in sides:
        s.own1[0].wait_recv()
        s.half1[0].start()
        start(s.cross[-1, 0])
        s.own1[1].wait_recv()
        start(s.cross[1, 0])
        s.own2[0].wait_recv()
        s.far[0, 0].start()
        s.own2[1].wait_recv()
    attend([[(0, -1, 0), (0, 1, 0), (-1, 0, 0), (1, 0, 0)]])
    for s in sides:
        s.z1[0].wait_recv()
        start(s.cross[-1, 1])
        s.z1[1].wait_recv()
        s.half1[1].start()
        start(s.cross[1, 1])
        s.z2[0].wait_recv()
        s.z2[1].wait_recv()
        s.far[0, 1].start()
    attend([[(0, -1, 1), (0, 1, 1), (-1, 0, 1), (1, 0, 1)]])

    def relay(r, k):
        for s in sides:
            for copy in s.cross[r, k]:
                copy.wait_recv()
            s.far[r, k].start()

    for s in sides:
        s.half1[0].wait_recv()
        start(s.cross[2, 0])
    relay(-1, 0)
    relay(1, 0)
    attend([[(di, dj, 0) for di in (-1, 1) for dj in (-1, 1)]])
    for s in sides:
        s.half1[1].wait_recv()
        start(s.cross[2, 1])
    attend([[(0, 0, 0), (0, 0, 1), (0, 2, 0), (0, 2, 1)]])
    relay(-1, 1)
    relay(1, 1)
    last_groups = [
        [(di, dj, 1) for di in (-1, 1) for dj in (-1, 1)],
        [(di, 2, k) for di in (-1, 1) for k in range(2)],
        [(2, r, k) for r in (0, -1) for k in range(2)],
        [(2, r, k) for r in (1, 2) for k in range(2)],
    ]
    attend(last_groups[0:1], 1 - zhi)
    relay(2, 0)
    relay(2, 1)
    attend(last_groups[1:2], 1 - zhi)
    for group, rs in ((2, (0, -1)), (3, (1, 2))):
        for s in sides:
            for r in rs:
                s.far[r, 0].wait_recv()
                s.far[r, 1].wait_recv()
        attend(last_groups[group : group + 1], 1 - zhi)

    def finish_attended(block):
        rows = pl.ds(pl.multiple_of(block * BLK, BLK), BLK)
        for h in range(heads):
            at = pl.ds(pl.multiple_of(block * span + h * BLK, BLK), BLK)
            att[rows, h * HEAD : (h + 1) * HEAD] = (
                (acc[0:HEAD, at] / acc[HEAD : HEAD + 1, at]).T
            ).astype(BF)

    finish_attended(1 - zhi)

    wcopies[3].wait()
    piece = BLK // 2
    mine = pl.ds(pl.multiple_of(core * piece, piece), piece)
    other = pl.ds(pl.multiple_of((1 - core) * piece, piece), piece)
    far_rows = pl.ds(pl.multiple_of((1 - zhi) * BLK, BLK), BLK)
    near_rows = pl.ds(pl.multiple_of(zhi * BLK, BLK), BLK)
    order = (0, 2, 1, 3)
    far_mate = [copy_to(d_out.at[j], d_in.at[j], mate) for j in range(4)]
    near_mate = [copy_to(dl_out.at[j], dl_in.at[j], mate) for j in range(4)]
    first_hop = [
        copy_to(zs_out.at[j], zr_rel.at[j], up if j < 2 else down) for j in range(4)
    ]
    second_hop = [
        copy_to(zr_rel.at[j], zr_in.at[j], up if j < 2 else down) for j in range(4)
    ]

    def pass_on(j):
        far_mate[j].wait_recv()
        zs_out[j] = (prem[j, mine, :] + d_in[j].astype(F32)).astype(BF)
        first_hop[j].start()

    last = None
    for j in order:
        prem[j] = dot(att[far_rows, :], wo[:, j * d : (j + 1) * d])
        d_out[j] = prem[j, other, :].astype(BF)
        far_mate[j].start()
        if last is not None:
            pass_on(last)
        last = j
    pass_on(last)
    for k in range(2):
        attend(last_groups[2 * k : 2 * k + 2], zhi)
        for j in order[2 * k : 2 * k + 2]:
            first_hop[j].wait_recv()
            second_hop[j].start()
    finish_attended(zhi)
    for j in order:
        ploc[j] = dot(att[near_rows, :], wo[:, j * d : (j + 1) * d])
        dl_out[j] = ploc[j, other, :].astype(BF)
        near_mate[j].start()
    for j in order:
        near_mate[j].wait_recv()
        ploc[j, mine, :] += dl_in[j].astype(F32)

    gate = 1.0 / (1.0 + jnp.exp(-gsum[zhi, mine, 0:1]))
    for j in order:
        second_hop[j].wait_recv()
    for ref, s in ((own, src_own), (part, src_mate), (zsame, src_same), (zother, src_other)):
        total = ploc[s, mine, :] + zr_in[s].astype(F32)
        out[:, pl.ds(pl.multiple_of(s * d, d), d)] = (ref[zhi, mine, :].astype(F32) + gate * total).astype(BF)

    for copy in made:
        copy.wait_send()


def on_device(resid, sel_blocks, norm_gain, router_weight, w_query, w_key, value_projection, w_out):
    local_rows, d = resid.shape
    width = w_out.shape[1]
    count = local_rows // BLK
    freqs = jnp.exp(
        jnp.arange(HEAD // 2, dtype=F32) * (-2.0 * math.log(rope_base) / HEAD)
    )
    freqs = jnp.concatenate([freqs, freqs]).reshape(1, HEAD)
    qcols = w_query.shape[1]
    heads = qcols // HEAD
    vmem = pl.BlockSpec(memory_space=pltpu.VMEM)
    anyspace = pl.BlockSpec(memory_space=pl.ANY)
    piece = BLK // 2
    nsem = 90
    result = pl.pallas_call(
        layer_kernel,
        name="layer",
        out_shape=jax.ShapeDtypeStruct((piece, width), BF),
        in_specs=[pl.BlockSpec(memory_space=pltpu.SMEM)] + [vmem] * 3 + [anyspace] * 5,
        out_specs=vmem,
        scratch_shapes=[
            pltpu.VMEM((count, BLK, d), BF),
            pltpu.VMEM((2, BLK, d), BF),
            pltpu.VMEM((2, BLK, HEAD), F32),
            pltpu.VMEM((2, BLK, HEAD), F32),
            pltpu.VMEM((width, qcols), BF),
            pltpu.VMEM((width, 2 * HEAD), BF),
            pltpu.VMEM((qcols, width), BF),
            pltpu.VMEM((2, BLK, d), BF),
            pltpu.VMEM((2, BLK, d), BF),
            pltpu.VMEM((2, BLK, d), BF),
            pltpu.VMEM((2, BLK, d // 2), BF),
            pltpu.VMEM((2, BLK, d // 2), BF),
            pltpu.VMEM((2, BLK, qcols), F32),
            pltpu.VMEM((2, BLK, 2 * HEAD), F32),
            pltpu.VMEM((2, BLK, HEAD), F32),
            pltpu.VMEM((2, BLK, HEAD), F32),
            pltpu.VMEM((heads * 256, HEAD), BF),
            pltpu.VMEM((8, 8 * BLK, 2 * HEAD), BF),
            pltpu.VMEM((8, heads * 256), F32),
            pltpu.VMEM((HEAD + 16, heads * 256), F32),
            pltpu.VMEM((2, 8 * BLK, 512), F32),
            pltpu.VMEM((2, 8 * BLK, 512), BF),
            pltpu.VMEM((2, 8, 512), F32),
            pltpu.VMEM((256, qcols), BF),
            pltpu.VMEM((4, BLK, d), F32),
            pltpu.VMEM((4, BLK, d), F32),
            pltpu.VMEM((4, piece, d), BF),
            pltpu.VMEM((4, piece, d), BF),
            pltpu.VMEM((4, piece, d), BF),
            pltpu.VMEM((4, piece, d), BF),
            pltpu.VMEM((4, piece, d), BF),
            pltpu.VMEM((4, piece, d), BF),
            pltpu.VMEM((4, piece, d), BF),
            pltpu.SemaphoreType.DMA((nsem,)),
            pltpu.SemaphoreType.DMA((nsem,)),
            pltpu.SemaphoreType.DMA((5,)),
        ],
        compiler_params=pltpu.CompilerParams(
            collective_id=0, has_side_effects=True, vmem_limit_bytes=60 * 1024 * 1024
        ),
    )(
        sel_blocks, freqs, norm_gain.reshape(1, width), router_weight.reshape(1, width),
        resid.reshape(count, BLK, d), w_query, w_key, value_projection, w_out,
    )
    return result


def solution(mesh):
    return jax.shard_map(
        on_device,
        mesh=mesh,
        in_specs=(
            P("ctx", "tp"),
            P("ctx"),
            P(),
            P(),
            P(None, "tp"),
            P(None, "tp"),
            P(None, "tp"),
            P("tp", None),
        ),
        out_specs=P(("ctx", "tp"), None),
        check_vma=False,
    )
```

```python
import math

import jax
import jax.numpy as jnp
import numpy as np
from jax import lax
from jax.experimental import pallas as pl
from jax.experimental.pallas import tpu as pltpu
from jax.sharding import PartitionSpec as P

HEAD = 128
BLK = 128
MESH = pl.DeviceIdType.MESH
BF = jnp.bfloat16
F32 = jnp.float32

rope_base = 500000.0
norm_eps = 1e-05
LOW = -1e30


def dot(a, b):
    return jnp.dot(a, b, preferred_element_type=F32)


def layer_kernel(
    sel, freq_hbm, gain_hbm, router_hbm, resid_hbm, wq_hbm, wk_hbm, wv_hbm, wo_hbm,
    out_hbm,
    freq, gain, router, out, resid, own, cosf, sinf, wq, wkv, wo, part, zsame, zother, rel_p, rel_m,
    qacc, kvacc, ssq, gsum, q, buf, m_ref, acc, s_ref, p_ref, x_ref, att,
    prem, ploc, d_out, d_in, dl_out, dl_in, zs_out, zr_rel, zr_in,
    ssem, rsem, wsem,
):
    c = lax.axis_index("ctx")
    t = lax.axis_index("tp")
    x, zlo, y = c // 8, (c // 4) % 2, c % 4
    zhi, core = t // 2, t % 2
    z = zhi * 2 + zlo
    d = own.shape[2]
    half = d // 2
    heads = q.shape[0] // 256
    width = wo.shape[1]
    nchunk = width // d

    def dev(dx=0, dy=0, dz=0, dc=0):
        nx, ny, nz = (x + dx + 4) % 4, (y + dy + 4) % 4, (z + dz + 4) % 4
        return (nx * 8 + (nz % 2) * 4 + ny, (nz // 2) * 2 + (core + dc) % 2)

    right_x, left_x = dev(dx=1), dev(dx=-1)
    right_y, left_y = dev(dy=1), dev(dy=-1)
    up, down = dev(dz=1), dev(dz=-1)
    mate = dev(dc=1)
    zpair = (x * 8 + (1 - zlo) * 4 + y, t)

    wcopies = [
        pltpu.make_async_copy(wq_hbm, wq, wsem.at[0]),
        pltpu.make_async_copy(wk_hbm, wkv.at[:, 0:HEAD], wsem.at[1]),
        pltpu.make_async_copy(wv_hbm, wkv.at[:, HEAD : 2 * HEAD], wsem.at[2]),
        pltpu.make_async_copy(wo_hbm, wo, wsem.at[3]),
    ]
    rcopy = pltpu.make_async_copy(resid_hbm, resid, wsem.at[4])
    small = [
        pltpu.make_async_copy(freq_hbm, freq, wsem.at[5]),
        pltpu.make_async_copy(gain_hbm, gain, wsem.at[6]),
        pltpu.make_async_copy(router_hbm, router, wsem.at[7]),
    ]
    barrier = pltpu.get_barrier_semaphore()
    for peer in (mate, up, down, right_x, left_x, right_y, left_y):
        pl.semaphore_signal(barrier, inc=1, device_id=peer, device_id_type=MESH)
    for copy in (rcopy, *small, *wcopies):
        copy.start()
    rcopy.wait()
    for b in range(2):
        at = jnp.clip(sel[b] - c * resid.shape[0], 0, resid.shape[0] - 1)
        own[b] = resid[at]
    pl.semaphore_wait(barrier, 7)

    made = []

    def copy_to(src, dst, peer):
        k = len(made)
        copy = pltpu.make_async_remote_copy(
            src_ref=src, dst_ref=dst, send_sem=ssem.at[k], recv_sem=rsem.at[k],
            device_id=peer, device_id_type=MESH,
        )
        made.append(copy)
        return copy

    to_mate = [copy_to(own.at[b], part.at[b], mate) for b in range(2)]
    to_up = [copy_to(own.at[b, :, 0:half], rel_p.at[b], up) for b in range(2)]
    to_down = [copy_to(own.at[b, :, half:d], rel_m.at[b], down) for b in range(2)]
    fwd_up = [copy_to(rel_p.at[b], zsame.at[b, :, 0:half], up) for b in range(2)]
    fwd_down = [copy_to(rel_m.at[b], zsame.at[b, :, half:d], down) for b in range(2)]
    fwd_mate = [copy_to(zsame.at[b], zother.at[b], mate) for b in range(2)]
    for b in range(2):
        to_up[b].start()
        to_down[b].start()
        to_mate[b].start()

    def rotated(v, b):
        return v * cosf[b] + pltpu.roll(v, HEAD // 2, 1) * sinf[b]

    def unit_at(base, i, j, k):
        return buf.at[base + i, pl.ds(pl.multiple_of((j * 2 + k) * BLK, BLK), BLK)]

    own_a = unit_at(0, y, x, zlo)
    own_b = unit_at(4, x, y, zlo)
    scale = math.log2(math.e) / math.sqrt(HEAD)
    span = heads * BLK

    def finish_keys(b):
        unit = own_b if b else own_a
        kv = kvacc[b] * lax.rsqrt(ssq[b][:, 0:1] * (1.0 / width) + norm_eps)
        unit[:, 0:HEAD] = rotated(kv[:, 0:HEAD], b).astype(BF)
        unit[:, HEAD : 2 * HEAD] = kv[:, HEAD:].T.astype(BF)

    def finish_queries(b):
        inv = lax.rsqrt(ssq[b][:, 0:1] * (1.0 / width) + norm_eps)
        for h in range(heads):
            qh = qacc[b][:, h * HEAD : (h + 1) * HEAD] * inv
            at = b * span + h * BLK
            q[at : at + BLK, :] = (rotated(qh, b) * scale).astype(BF)

    class Side:
        def __init__(self, base, i, j, plus1, minus1, plus2, minus2):
            self.base, self.i, self.j = base, i, j
            first, second = (plus1, minus1), (plus2, minus2)
            self.to_z = self.send(0, 0, 0, zpair)
            self.own1 = [self.send(0, 0, 0, peer) for peer in first]
            self.own2 = [self.send(0, 0, 0, peer) for peer in second]
            self.z1 = [self.send(0, 0, 1, peer) for peer in first]
            self.z2 = [self.send(0, 0, 1, peer) for peer in second]
            self.half1 = [self.send(0, -1, 0, plus1), self.send(0, 1, 1, minus1)]
            self.cross = {
                (r, k): [self.send(0, r, k, peer) for peer in second]
                for r in (-1, 1, 2)
                for k in range(2)
            }
            self.far = {
                (r, k): self.send(1 if k else -1, r, k, minus2 if k else plus2)
                for r in (0, -1, 1, 2)
                for k in range(2)
            }

        def place(self, di, dj, k):
            plane = 1 - zlo if k else zlo
            return lax.rem(self.i + di + 4, 4), lax.rem(self.j + dj + 4, 4), plane

        def unit(self, di, dj, k):
            return unit_at(self.base, *self.place(di, dj, k))

        def send(self, di, dj, k, peer):
            return copy_to(self.unit(di, dj, k), self.unit(di, dj, k), peer)

        def allowed(self, di, dj, k):
            i, j, plane = self.place(di, dj, k)
            return (i * 8 + j if self.base else j * 8 + i) + plane * 4 < c

    sides = (
        Side(0, y, x, right_x, left_x, right_y, left_y),
        Side(4, x, y, right_y, left_y, right_x, left_x),
    )

    def start(*groups):
        for group in groups:
            for copy in group:
                copy.start()

    for copy in small:
        copy.wait()
    lane = lax.broadcasted_iota(jnp.int32, (BLK, HEAD), 1)
    row = lax.broadcasted_iota(jnp.int32, (BLK, HEAD), 0)
    for b in range(2):
        angle = (row + sel[b] * BLK).astype(F32) * freq[...]
        cosf[b] = jnp.cos(angle)
        sine = jnp.sin(angle)
        sinf[b] = jnp.where(lane < HEAD // 2, -sine, sine)
    ssq[...] = jnp.zeros_like(ssq)
    gsum[...] = jnp.zeros_like(gsum)
    src_own, src_mate = t, t + 1 - 2 * core
    src_same = (t + 2) % 4
    src_other = (src_mate + 2) % 4

    def project(ref, b, s, first=False):
        rows = pl.ds(pl.multiple_of(s * d, d), d)
        ch = ref[b].astype(F32)
        ssq[b] += jnp.broadcast_to(jnp.sum(ch * ch, axis=1, keepdims=True), (BLK, HEAD))
        gsum[b] += jnp.broadcast_to(
            jnp.sum(ch * router[:, rows], axis=1, keepdims=True), (BLK, HEAD)
        )
        cg = (ch * gain[:, rows]).astype(BF)

        def into(total, weight):
            part_sum = dot(cg, weight[rows, :])
            if first:
                total[b] = part_sum
            else:
                total[b] += part_sum

        into(kvacc, wkv)
        return lambda: into(qacc, wq)

    def relay_features(b):
        to_up[b].wait_recv()
        fwd_up[b].start()
        to_down[b].wait_recv()
        fwd_down[b].start()

    relay_features(0)
    for copy in wcopies[:3]:
        copy.wait()
    for b in range(2):
        project(own, b, src_own, True)()
    relay_features(1)
    for b in range(2):
        to_mate[b].wait_recv()
        project(part, b, src_mate)()
    for b in range(2):
        fwd_up[b].wait_recv()
        fwd_down[b].wait_recv()
        fwd_mate[b].start()
        project(zsame, b, src_same)()
        fwd_mate[b].wait_recv()
        rest = project(zother, b, src_other)
        finish_keys(b)
        sides[b].to_z.start()
        start(sides[b].own1, sides[b].own2)
        rest()
        finish_queries(b)

    cols = 512
    tiles = span // cols
    ones_rows = jnp.ones((16, 8 * BLK), BF)

    def scores_of(ks, at):
        return lax.dot_general(
            ks, q[at, :], (((1,), (1,)), ((), ())), preferred_element_type=F32
        )

    keys_own = jnp.concatenate([own_a[:, 0:HEAD], own_b[:, 0:HEAD]], axis=0)
    v_own = jnp.concatenate([own_a[:, HEAD:], own_b[:, HEAD:]], axis=1)
    v_own = jnp.concatenate([v_own, ones_rows[:, 0 : 2 * BLK]], axis=0)
    key_at = lax.broadcasted_iota(jnp.int32, (256, cols), 0)
    query_at = lax.broadcasted_iota(jnp.int32, (256, cols), 1) & (BLK - 1)
    for r in range(2 * tiles):
        at = slice(r * cols, (r + 1) * cols)
        seen = key_at <= query_at + (r // tiles) * BLK
        sc = jnp.where(seen, scores_of(keys_own, at), LOW)
        high = jnp.max(sc, axis=0, keepdims=True)
        pr = jnp.where(seen, jnp.exp2(sc - high), 0.0).astype(BF)
        m_ref[:, at] = jnp.broadcast_to(high, (8, cols))
        acc[:, at] = dot(v_own, pr)

    def attend(groups, block=None):
        units = [[(s, p) for s in sides for p in places] for places in groups]
        allowed = [[s.allowed(*p) for s, p in group] for group in units]
        some = allowed[0][0]
        for flags in allowed:
            for flag in flags:
                some = jnp.logical_or(some, flag)
        if block is None:
            spots = [slice(r * cols, (r + 1) * cols) for r in range(2 * tiles)]
        else:
            spots = [
                pl.ds(pl.multiple_of(block * span + r * cols, cols), cols)
                for r in range(tiles)
            ]
        steps = [(g, at) for g in range(len(groups)) for at in spots]

        @pl.when(some)
        def _():
            def score(k):
                g, at = steps[k]
                ks = jnp.concatenate([s.unit(*p)[:, 0:HEAD] for s, p in units[g]], axis=0)
                sc = scores_of(ks, at)
                s_ref[k % 2] = jnp.concatenate(
                    [
                        sc[u * BLK : (u + 1) * BLK] + jnp.where(allowed[g][u], 0.0, LOW)
                        for u in range(8)
                    ],
                    axis=0,
                )

            def soften(k):
                at = steps[k][1]
                sc = s_ref[k % 2]
                old = m_ref[0:1, at]
                high = jnp.maximum(old, jnp.max(sc, axis=0, keepdims=True))
                p_ref[k % 2] = jnp.exp2(sc - high).astype(BF)
                x_ref[k % 2] = jnp.broadcast_to(jnp.exp2(old - high), (8, cols))
                m_ref[:, at] = jnp.broadcast_to(high, (8, cols))

            def collect(k):
                g, at = steps[k]
                vt = jnp.concatenate([s.unit(*p)[:, HEAD:] for s, p in units[g]], axis=1)
                vt = jnp.concatenate([vt, ones_rows], axis=0)
                acc[:, at] = acc[:, at] * x_ref[k % 2][0:1] + dot(vt, p_ref[k % 2])

            count = len(steps)
            for k in range(count + 2):
                if k < count:
                    score(k)
                if k >= 2:
                    collect(k - 2)
                if 1 <= k <= count:
                    soften(k - 1)

    for s in sides:
        s.to_z.wait_recv()
        start(s.z1, s.z2)
    for s in sides:
        s.own1[0].wait_recv()
        s.half1[0].start()
        start(s.cross[-1, 0])
        s.own1[1].wait_recv()
        start(s.cross[1, 0])
        s.own2[0].wait_recv()
        s.far[0, 0].start()
        s.own2[1].wait_recv()
    attend([[(0, -1, 0), (0, 1, 0), (-1, 0, 0), (1, 0, 0)]])
    for s in sides:
        s.z1[0].wait_recv()
        start(s.cross[-1, 1])
        s.z1[1].wait_recv()
        s.half1[1].start()
        start(s.cross[1, 1])
        s.z2[0].wait_recv()
        s.z2[1].wait_recv()
        s.far[0, 1].start()
    attend([[(0, -1, 1), (0, 1, 1), (-1, 0, 1), (1, 0, 1)]])

    def relay(r, k):
        for s in sides:
            for copy in s.cross[r, k]:
                copy.wait_recv()
            s.far[r, k].start()

    for s in sides:
        s.half1[0].wait_recv()
        start(s.cross[2, 0])
    relay(-1, 0)
    relay(1, 0)
    attend([[(di, dj, 0) for di in (-1, 1) for dj in (-1, 1)]])
    for s in sides:
        s.half1[1].wait_recv()
        start(s.cross[2, 1])
    attend([[(0, 0, 0), (0, 0, 1), (0, 2, 0), (0, 2, 1)]])
    relay(-1, 1)
    relay(1, 1)
    last_groups = [
        [(di, dj, 1) for di in (-1, 1) for dj in (-1, 1)],
        [(di, 2, k) for di in (-1, 1) for k in range(2)],
        [(2, r, k) for r in (0, -1) for k in range(2)],
        [(2, r, k) for r in (1, 2) for k in range(2)],
    ]
    attend(last_groups[0:1], 1 - zhi)
    relay(2, 0)
    relay(2, 1)
    attend(last_groups[1:2], 1 - zhi)
    for group, rs in ((2, (0, -1)), (3, (1, 2))):
        for s in sides:
            for r in rs:
                s.far[r, 0].wait_recv()
                s.far[r, 1].wait_recv()
        attend(last_groups[group : group + 1], 1 - zhi)

    def finish_attended(block):
        rows = pl.ds(pl.multiple_of(block * BLK, BLK), BLK)
        for h in range(heads):
            at = pl.ds(pl.multiple_of(block * span + h * BLK, BLK), BLK)
            att[rows, h * HEAD : (h + 1) * HEAD] = (
                (acc[0:HEAD, at] / acc[HEAD : HEAD + 1, at]).T
            ).astype(BF)

    finish_attended(1 - zhi)

    wcopies[3].wait()
    piece = BLK // 2
    mine = pl.ds(pl.multiple_of(core * piece, piece), piece)
    other = pl.ds(pl.multiple_of((1 - core) * piece, piece), piece)
    far_rows = pl.ds(pl.multiple_of((1 - zhi) * BLK, BLK), BLK)
    near_rows = pl.ds(pl.multiple_of(zhi * BLK, BLK), BLK)
    order = (0, 2, 1, 3)
    far_mate = [copy_to(d_out.at[j], d_in.at[j], mate) for j in range(4)]
    near_mate = [copy_to(dl_out.at[j], dl_in.at[j], mate) for j in range(4)]
    first_hop = [
        copy_to(zs_out.at[j], zr_rel.at[j], up if j < 2 else down) for j in range(4)
    ]
    second_hop = [
        copy_to(zr_rel.at[j], zr_in.at[j], up if j < 2 else down) for j in range(4)
    ]

    def pass_on(j):
        far_mate[j].wait_recv()
        zs_out[j] = (prem[j, mine, :] + d_in[j].astype(F32)).astype(BF)
        first_hop[j].start()

    last = None
    for j in order:
        prem[j] = dot(att[far_rows, :], wo[:, j * d : (j + 1) * d])
        d_out[j] = prem[j, other, :].astype(BF)
        far_mate[j].start()
        if last is not None:
            pass_on(last)
        last = j
    pass_on(last)
    for k in range(2):
        attend(last_groups[2 * k : 2 * k + 2], zhi)
        for j in order[2 * k : 2 * k + 2]:
            first_hop[j].wait_recv()
            second_hop[j].start()
    finish_attended(zhi)
    for j in order:
        ploc[j] = dot(att[near_rows, :], wo[:, j * d : (j + 1) * d])
        dl_out[j] = ploc[j, other, :].astype(BF)
        near_mate[j].start()
    for j in order:
        near_mate[j].wait_recv()

    gate = 1.0 / (1.0 + jnp.exp(-gsum[zhi, mine, 0:1]))
    for ref, s in ((own, src_own), (part, src_mate), (zsame, src_same), (zother, src_other)):
        ploc[s, mine, :] = ref[zhi, mine, :].astype(F32) + gate * (
            ploc[s, mine, :] + dl_in[s].astype(F32)
        )
    outs = [
        pltpu.make_async_copy(
            out.at[:, j * d : (j + 1) * d], out_hbm.at[:, j * d : (j + 1) * d], wsem.at[8 + j]
        )
        for j in range(4)
    ]
    for j in order:
        second_hop[j].wait_recv()
        out[:, j * d : (j + 1) * d] = (
            ploc[j, mine, :] + gate * zr_in[j].astype(F32)
        ).astype(BF)
        outs[j].start()

    for copy in outs:
        copy.wait()
    for copy in made:
        copy.wait_send()


def on_device(resid, sel_blocks, norm_gain, router_weight, w_query, w_key, value_projection, w_out):
    local_rows, d = resid.shape
    width = w_out.shape[1]
    count = local_rows // BLK
    powers = np.arange(HEAD // 2, dtype=np.float32) * np.float32(
        -2.0 * math.log(rope_base) / HEAD
    )
    freqs = jnp.asarray(np.tile(np.exp(powers), 2).reshape(1, HEAD), F32)
    qcols = w_query.shape[1]
    heads = qcols // HEAD
    anyspace = pl.BlockSpec(memory_space=pltpu.HBM)
    piece = BLK // 2
    nsem = 90
    result = pl.pallas_call(
        layer_kernel,
        name="layer",
        out_shape=jax.ShapeDtypeStruct((piece, width), BF),
        in_specs=[pl.BlockSpec(memory_space=pltpu.SMEM)] + [anyspace] * 8,
        out_specs=anyspace,
        scratch_shapes=[
            pltpu.VMEM((1, HEAD), F32),
            pltpu.VMEM((1, width), F32),
            pltpu.VMEM((1, width), F32),
            pltpu.VMEM((piece, width), BF),
            pltpu.VMEM((count, BLK, d), BF),
            pltpu.VMEM((2, BLK, d), BF),
            pltpu.VMEM((2, BLK, HEAD), F32),
            pltpu.VMEM((2, BLK, HEAD), F32),
            pltpu.VMEM((width, qcols), BF),
            pltpu.VMEM((width, 2 * HEAD), BF),
            pltpu.VMEM((qcols, width), BF),
            pltpu.VMEM((2, BLK, d), BF),
            pltpu.VMEM((2, BLK, d), BF),
            pltpu.VMEM((2, BLK, d), BF),
            pltpu.VMEM((2, BLK, d // 2), BF),
            pltpu.VMEM((2, BLK, d // 2), BF),
            pltpu.VMEM((2, BLK, qcols), F32),
            pltpu.VMEM((2, BLK, 2 * HEAD), F32),
            pltpu.VMEM((2, BLK, HEAD), F32),
            pltpu.VMEM((2, BLK, HEAD), F32),
            pltpu.VMEM((heads * 256, HEAD), BF),
            pltpu.VMEM((8, 8 * BLK, 2 * HEAD), BF),
            pltpu.VMEM((8, heads * 256), F32),
            pltpu.VMEM((HEAD + 16, heads * 256), F32),
            pltpu.VMEM((2, 8 * BLK, 512), F32),
            pltpu.VMEM((2, 8 * BLK, 512), BF),
            pltpu.VMEM((2, 8, 512), F32),
            pltpu.VMEM((256, qcols), BF),
            pltpu.VMEM((4, BLK, d), F32),
            pltpu.VMEM((4, BLK, d), F32),
            pltpu.VMEM((4, piece, d), BF),
            pltpu.VMEM((4, piece, d), BF),
            pltpu.VMEM((4, piece, d), BF),
            pltpu.VMEM((4, piece, d), BF),
            pltpu.VMEM((4, piece, d), BF),
            pltpu.VMEM((4, piece, d), BF),
            pltpu.VMEM((4, piece, d), BF),
            pltpu.SemaphoreType.DMA((nsem,)),
            pltpu.SemaphoreType.DMA((nsem,)),
            pltpu.SemaphoreType.DMA((12,)),
        ],
        compiler_params=pltpu.CompilerParams(
            collective_id=0, has_side_effects=True, vmem_limit_bytes=54 * 1024 * 1024
        ),
    )(
        sel_blocks, freqs, norm_gain.reshape(1, width), router_weight.reshape(1, width),
        resid.reshape(count, BLK, d), w_query, w_key, value_projection, w_out,
    )
    return result


def solution(mesh):
    return jax.shard_map(
        on_device,
        mesh=mesh,
        in_specs=(
            P("ctx", "tp"),
            P("ctx"),
            P(),
            P(),
            P(None, "tp"),
            P(None, "tp"),
            P(None, "tp"),
            P("tp", None),
        ),
        out_specs=P(("ctx", "tp"), None),
        check_vma=False,
    )
```

```python
import math

import jax
import jax.numpy as jnp
import numpy as np
from jax import lax
from jax.experimental import pallas as pl
from jax.experimental.pallas import tpu as pltpu
from jax.sharding import PartitionSpec as P

HEAD = 128
BLK = 128
MESH = pl.DeviceIdType.MESH
BF = jnp.bfloat16
F32 = jnp.float32

rope_base = 500000.0
norm_eps = 1e-05
LOW = -1e30


def dot(a, b):
    return jnp.dot(a, b, preferred_element_type=F32)


def layer_kernel(
    sel, freq_hbm, gain_hbm, router_hbm, resid_hbm, wq_hbm, wk_hbm, wv_hbm, wo_hbm,
    out_hbm,
    freq, gain, router, out, resid, own, cosf, sinf, wq, wkv, wo, part, zsame, zother, rel_p, rel_m,
    qacc, kvacc, ssq, gsum, q, buf, m_ref, acc, s_ref, p_ref, x_ref, att,
    prem, ploc, d_out, d_in, dl_out, dl_in, zs_out, zr_rel, zr_in,
    ssem, rsem, wsem,
):
    c = lax.axis_index("ctx")
    t = lax.axis_index("tp")
    x, zlo, y = c // 8, (c // 4) % 2, c % 4
    zhi, core = t // 2, t % 2
    z = zhi * 2 + zlo
    d = own.shape[2]
    half = d // 2
    heads = q.shape[0] // 256
    width = wo.shape[1]
    nchunk = width // d

    def dev(dx=0, dy=0, dz=0, dc=0):
        nx, ny, nz = (x + dx + 4) % 4, (y + dy + 4) % 4, (z + dz + 4) % 4
        return (nx * 8 + (nz % 2) * 4 + ny, (nz // 2) * 2 + (core + dc) % 2)

    right_x, left_x = dev(dx=1), dev(dx=-1)
    right_y, left_y = dev(dy=1), dev(dy=-1)
    up, down = dev(dz=1), dev(dz=-1)
    mate = dev(dc=1)
    zpair = (x * 8 + (1 - zlo) * 4 + y, t)

    wcopies = [
        pltpu.make_async_copy(wq_hbm, wq, wsem.at[0]),
        pltpu.make_async_copy(wk_hbm, wkv.at[:, 0:HEAD], wsem.at[1]),
        pltpu.make_async_copy(wv_hbm, wkv.at[:, HEAD : 2 * HEAD], wsem.at[2]),
        pltpu.make_async_copy(wo_hbm, wo, wsem.at[3]),
    ]
    rcopy = pltpu.make_async_copy(resid_hbm, resid, wsem.at[4])
    small = [
        pltpu.make_async_copy(freq_hbm, freq, wsem.at[5]),
        pltpu.make_async_copy(gain_hbm, gain, wsem.at[6]),
        pltpu.make_async_copy(router_hbm, router, wsem.at[7]),
    ]
    barrier = pltpu.get_barrier_semaphore()
    for peer in (mate, up, down, right_x, left_x, right_y, left_y):
        pl.semaphore_signal(barrier, inc=1, device_id=peer, device_id_type=MESH)
    for copy in (rcopy, *small, *wcopies):
        copy.start()
    rcopy.wait()
    for b in range(2):
        at = jnp.clip(sel[b] - c * resid.shape[0], 0, resid.shape[0] - 1)
        own[b] = resid[at]
    pl.semaphore_wait(barrier, 7)

    made = []

    def copy_to(src, dst, peer):
        k = len(made)
        copy = pltpu.make_async_remote_copy(
            src_ref=src, dst_ref=dst, send_sem=ssem.at[k], recv_sem=rsem.at[k],
            device_id=peer, device_id_type=MESH,
        )
        made.append(copy)
        return copy

    to_mate = [copy_to(own.at[b], part.at[b], mate) for b in range(2)]
    to_up = [copy_to(own.at[b, :, 0:half], rel_p.at[b], up) for b in range(2)]
    to_down = [copy_to(own.at[b, :, half:d], rel_m.at[b], down) for b in range(2)]
    fwd_up = [copy_to(rel_p.at[b], zsame.at[b, :, 0:half], up) for b in range(2)]
    fwd_down = [copy_to(rel_m.at[b], zsame.at[b, :, half:d], down) for b in range(2)]
    fwd_mate = [copy_to(zsame.at[b], zother.at[b], mate) for b in range(2)]
    for b in range(2):
        to_up[b].start()
        to_down[b].start()
        to_mate[b].start()

    def rotated(v, b):
        return v * cosf[b] + pltpu.roll(v, HEAD // 2, 1) * sinf[b]

    def unit_at(base, i, j, k):
        return buf.at[base + i, pl.ds(pl.multiple_of((j * 2 + k) * BLK, BLK), BLK)]

    own_a = unit_at(0, y, x, zlo)
    own_b = unit_at(4, x, y, zlo)
    scale = math.log2(math.e) / math.sqrt(HEAD)
    span = heads * BLK

    def finish_keys(b):
        unit = own_b if b else own_a
        kv = kvacc[b] * lax.rsqrt(ssq[b][:, 0:1] * (1.0 / width) + norm_eps)
        unit[:, 0:HEAD] = rotated(kv[:, 0:HEAD], b).astype(BF)
        unit[:, HEAD : 2 * HEAD] = kv[:, HEAD:].T.astype(BF)

    def finish_queries(b):
        inv = lax.rsqrt(ssq[b][:, 0:1] * (1.0 / width) + norm_eps)
        for h in range(heads):
            qh = qacc[b][:, h * HEAD : (h + 1) * HEAD] * inv
            at = b * span + h * BLK
            q[at : at + BLK, :] = (rotated(qh, b) * scale).astype(BF)

    class Side:
        def __init__(self, base, i, j, plus1, minus1, plus2, minus2):
            self.base, self.i, self.j = base, i, j
            first, second = (plus1, minus1), (plus2, minus2)
            self.to_z = self.send(0, 0, 0, zpair)
            self.own1 = [self.send(0, 0, 0, peer) for peer in first]
            self.own2 = [self.send(0, 0, 0, peer) for peer in second]
            self.z1 = [self.send(0, 0, 1, peer) for peer in first]
            self.z2 = [self.send(0, 0, 1, peer) for peer in second]
            self.half1 = [self.send(0, -1, 0, plus1), self.send(0, 1, 1, minus1)]
            self.cross = {
                (r, k): [self.send(0, r, k, peer) for peer in second]
                for r in (-1, 1, 2)
                for k in range(2)
            }
            self.far = {
                (r, k): self.send(1 if k else -1, r, k, minus2 if k else plus2)
                for r in (0, -1, 1, 2)
                for k in range(2)
            }

        def place(self, di, dj, k):
            plane = 1 - zlo if k else zlo
            return lax.rem(self.i + di + 4, 4), lax.rem(self.j + dj + 4, 4), plane

        def unit(self, di, dj, k):
            return unit_at(self.base, *self.place(di, dj, k))

        def send(self, di, dj, k, peer):
            return copy_to(self.unit(di, dj, k), self.unit(di, dj, k), peer)

        def allowed(self, di, dj, k):
            i, j, plane = self.place(di, dj, k)
            return (i * 8 + j if self.base else j * 8 + i) + plane * 4 < c

    sides = (
        Side(0, y, x, right_x, left_x, right_y, left_y),
        Side(4, x, y, right_y, left_y, right_x, left_x),
    )

    def start(*groups):
        for group in groups:
            for copy in group:
                copy.start()

    for copy in small:
        copy.wait()
    lane = lax.broadcasted_iota(jnp.int32, (BLK, HEAD), 1)
    row = lax.broadcasted_iota(jnp.int32, (BLK, HEAD), 0)
    for b in range(2):
        angle = (row + sel[b] * BLK).astype(F32) * freq[...]
        cosf[b] = jnp.cos(angle)
        sine = jnp.sin(angle)
        sinf[b] = jnp.where(lane < HEAD // 2, -sine, sine)
    ssq[...] = jnp.zeros_like(ssq)
    gsum[...] = jnp.zeros_like(gsum)
    src_own, src_mate = t, t + 1 - 2 * core
    src_same = (t + 2) % 4
    src_other = (src_mate + 2) % 4

    def project(ref, b, s, first=False):
        rows = pl.ds(pl.multiple_of(s * d, d), d)
        ch = ref[b].astype(F32)
        ssq[b] += jnp.broadcast_to(jnp.sum(ch * ch, axis=1, keepdims=True), (BLK, HEAD))
        gsum[b] += jnp.broadcast_to(
            jnp.sum(ch * router[:, rows], axis=1, keepdims=True), (BLK, HEAD)
        )
        cg = (ch * gain[:, rows]).astype(BF)

        def into(total, weight):
            part_sum = dot(cg, weight[rows, :])
            if first:
                total[b] = part_sum
            else:
                total[b] += part_sum

        into(kvacc, wkv)
        return lambda: into(qacc, wq)

    def relay_features(b):
        to_up[b].wait_recv()
        fwd_up[b].start()
        to_down[b].wait_recv()
        fwd_down[b].start()

    relay_features(0)
    for copy in wcopies[:3]:
        copy.wait()
    for b in range(2):
        project(own, b, src_own, True)()
    relay_features(1)
    for b in range(2):
        to_mate[b].wait_recv()
        project(part, b, src_mate)()
    for b in range(2):
        fwd_up[b].wait_recv()
        fwd_down[b].wait_recv()
        fwd_mate[b].start()
        project(zsame, b, src_same)()
        fwd_mate[b].wait_recv()
        rest = project(zother, b, src_other)
        finish_keys(b)
        sides[b].to_z.start()
        start(sides[b].own1, sides[b].own2)
        rest()
        finish_queries(b)

    cols = 512
    tiles = span // cols
    ones_rows = jnp.ones((16, 8 * BLK), BF)

    def scores_of(ks, at):
        return lax.dot_general(
            ks, q[at, :], (((1,), (1,)), ((), ())), preferred_element_type=F32
        )

    keys_own = jnp.concatenate([own_a[:, 0:HEAD], own_b[:, 0:HEAD]], axis=0)
    v_own = jnp.concatenate([own_a[:, HEAD:], own_b[:, HEAD:]], axis=1)
    v_own = jnp.concatenate([v_own, ones_rows[:, 0 : 2 * BLK]], axis=0)
    key_at = lax.broadcasted_iota(jnp.int32, (256, cols), 0)
    query_at = lax.broadcasted_iota(jnp.int32, (256, cols), 1) & (BLK - 1)
    for r in range(2 * tiles):
        at = slice(r * cols, (r + 1) * cols)
        seen = key_at <= query_at + (r // tiles) * BLK
        sc = jnp.where(seen, scores_of(keys_own, at), LOW)
        high = jnp.max(sc, axis=0, keepdims=True)
        pr = jnp.where(seen, jnp.exp2(sc - high), 0.0).astype(BF)
        m_ref[:, at] = jnp.broadcast_to(high, (8, cols))
        acc[:, at] = dot(v_own, pr)

    def attend(groups, block=None):
        units = [[(s, p) for s in sides for p in places] for places in groups]
        allowed = [[s.allowed(*p) for s, p in group] for group in units]
        some = allowed[0][0]
        for flags in allowed:
            for flag in flags:
                some = jnp.logical_or(some, flag)
        if block is None:
            spots = [slice(r * cols, (r + 1) * cols) for r in range(2 * tiles)]
        else:
            spots = [
                pl.ds(pl.multiple_of(block * span + r * cols, cols), cols)
                for r in range(tiles)
            ]
        steps = [(g, at) for g in range(len(groups)) for at in spots]

        @pl.when(some)
        def _():
            def score(k):
                g, at = steps[k]
                ks = jnp.concatenate([s.unit(*p)[:, 0:HEAD] for s, p in units[g]], axis=0)
                sc = scores_of(ks, at)
                s_ref[k % 2] = jnp.concatenate(
                    [
                        sc[u * BLK : (u + 1) * BLK] + jnp.where(allowed[g][u], 0.0, LOW)
                        for u in range(8)
                    ],
                    axis=0,
                )

            def soften(k):
                at = steps[k][1]
                sc = s_ref[k % 2]
                old = m_ref[0:1, at]
                high = jnp.maximum(old, jnp.max(sc, axis=0, keepdims=True))
                p_ref[k % 2] = jnp.exp2(sc - high).astype(BF)
                x_ref[k % 2] = jnp.broadcast_to(jnp.exp2(old - high), (8, cols))
                m_ref[:, at] = jnp.broadcast_to(high, (8, cols))

            def collect(k):
                g, at = steps[k]
                vt = jnp.concatenate([s.unit(*p)[:, HEAD:] for s, p in units[g]], axis=1)
                vt = jnp.concatenate([vt, ones_rows], axis=0)
                acc[:, at] = acc[:, at] * x_ref[k % 2][0:1] + dot(vt, p_ref[k % 2])

            count = len(steps)
            for k in range(count + 2):
                if k < count:
                    score(k)
                if k >= 2:
                    collect(k - 2)
                if 1 <= k <= count:
                    soften(k - 1)

    for s in sides:
        s.to_z.wait_recv()
        start(s.z1, s.z2)
    for s in sides:
        s.own1[0].wait_recv()
        s.half1[0].start()
        start(s.cross[-1, 0])
        s.own1[1].wait_recv()
        start(s.cross[1, 0])
        s.own2[0].wait_recv()
        s.far[0, 0].start()
        s.own2[1].wait_recv()
    attend([[(0, -1, 0), (0, 1, 0), (-1, 0, 0), (1, 0, 0)]])
    for s in sides:
        s.z1[0].wait_recv()
        start(s.cross[-1, 1])
        s.z1[1].wait_recv()
        s.half1[1].start()
        start(s.cross[1, 1])
        s.z2[0].wait_recv()
        s.z2[1].wait_recv()
        s.far[0, 1].start()
    attend([[(0, -1, 1), (0, 1, 1), (-1, 0, 1), (1, 0, 1)]])

    def relay(r, k):
        for s in sides:
            for copy in s.cross[r, k]:
                copy.wait_recv()
            s.far[r, k].start()

    for s in sides:
        s.half1[0].wait_recv()
        start(s.cross[2, 0])
    relay(-1, 0)
    relay(1, 0)
    attend([[(di, dj, 0) for di in (-1, 1) for dj in (-1, 1)]])
    for s in sides:
        s.half1[1].wait_recv()
        start(s.cross[2, 1])
    relay(-1, 1)
    relay(1, 1)
    attend([[(0, 0, 0), (0, 0, 1), (0, 2, 0), (0, 2, 1)]])
    last_groups = [
        [(di, dj, 1) for di in (-1, 1) for dj in (-1, 1)],
        [(di, 2, k) for di in (-1, 1) for k in range(2)],
        [(2, r, k) for r in (0, -1) for k in range(2)],
        [(2, r, k) for r in (1, 2) for k in range(2)],
    ]
    attend(last_groups[0:1], 1 - zhi)
    relay(2, 0)
    relay(2, 1)
    attend(last_groups[1:2], 1 - zhi)
    for group, rs in ((2, (0, -1)), (3, (1, 2))):
        for s in sides:
            for r in rs:
                s.far[r, 0].wait_recv()
                s.far[r, 1].wait_recv()
        attend(last_groups[group : group + 1], 1 - zhi)

    def finish_attended(block):
        rows = pl.ds(pl.multiple_of(block * BLK, BLK), BLK)
        for h in range(heads):
            at = pl.ds(pl.multiple_of(block * span + h * BLK, BLK), BLK)
            att[rows, h * HEAD : (h + 1) * HEAD] = (
                (acc[0:HEAD, at] / acc[HEAD : HEAD + 1, at]).T
            ).astype(BF)

    finish_attended(1 - zhi)

    wcopies[3].wait()
    piece = BLK // 2
    mine = pl.ds(pl.multiple_of(core * piece, piece), piece)
    other = pl.ds(pl.multiple_of((1 - core) * piece, piece), piece)
    far_rows = pl.ds(pl.multiple_of((1 - zhi) * BLK, BLK), BLK)
    near_rows = pl.ds(pl.multiple_of(zhi * BLK, BLK), BLK)
    order = (0, 2, 1, 3)
    far_mate = [copy_to(d_out.at[j], d_in.at[j], mate) for j in range(4)]
    near_mate = [copy_to(dl_out.at[j], dl_in.at[j], mate) for j in range(4)]
    first_hop = [
        copy_to(zs_out.at[j], zr_rel.at[j], up if j < 2 else down) for j in range(4)
    ]
    second_hop = [
        copy_to(zr_rel.at[j], zr_in.at[j], up if j < 2 else down) for j in range(4)
    ]

    def pass_on(j):
        far_mate[j].wait_recv()
        zs_out[j] = (prem[j, mine, :] + d_in[j].astype(F32)).astype(BF)
        first_hop[j].start()

    last = None
    for j in order:
        prem[j] = dot(att[far_rows, :], wo[:, j * d : (j + 1) * d])
        d_out[j] = prem[j, other, :].astype(BF)
        far_mate[j].start()
        if last is not None:
            pass_on(last)
        last = j
    pass_on(last)
    for k in range(2):
        attend(last_groups[2 * k : 2 * k + 2], zhi)
        for j in order[2 * k : 2 * k + 2]:
            first_hop[j].wait_recv()
            second_hop[j].start()
    finish_attended(zhi)
    for j in order:
        ploc[j] = dot(att[near_rows, :], wo[:, j * d : (j + 1) * d])
        dl_out[j] = ploc[j, other, :].astype(BF)
        near_mate[j].start()
    for j in order:
        near_mate[j].wait_recv()

    gate = 1.0 / (1.0 + jnp.exp(-gsum[zhi, mine, 0:1]))
    for ref, s in ((own, src_own), (part, src_mate), (zsame, src_same), (zother, src_other)):
        ploc[s, mine, :] = ref[zhi, mine, :].astype(F32) + gate * (
            ploc[s, mine, :] + dl_in[s].astype(F32)
        )
    outs = [
        pltpu.make_async_copy(
            out.at[:, j * d : (j + 1) * d], out_hbm.at[:, j * d : (j + 1) * d], wsem.at[8 + j]
        )
        for j in range(4)
    ]
    for j in order:
        second_hop[j].wait_recv()
        out[:, j * d : (j + 1) * d] = (
            ploc[j, mine, :] + gate * zr_in[j].astype(F32)
        ).astype(BF)
        outs[j].start()

    for copy in outs:
        copy.wait()
    for copy in made:
        copy.wait_send()


def on_device(resid, sel_blocks, norm_gain, router_weight, w_query, w_key, value_projection, w_out):
    local_rows, d = resid.shape
    width = w_out.shape[1]
    count = local_rows // BLK
    powers = np.arange(HEAD // 2, dtype=np.float32) * np.float32(
        -2.0 * math.log(rope_base) / HEAD
    )
    freqs = jnp.asarray(np.tile(np.exp(powers), 2).reshape(1, HEAD), F32)
    qcols = w_query.shape[1]
    heads = qcols // HEAD
    anyspace = pl.BlockSpec(memory_space=pltpu.HBM)
    piece = BLK // 2
    nsem = 90
    result = pl.pallas_call(
        layer_kernel,
        name="layer",
        out_shape=jax.ShapeDtypeStruct((piece, width), BF),
        in_specs=[pl.BlockSpec(memory_space=pltpu.SMEM)] + [anyspace] * 8,
        out_specs=anyspace,
        scratch_shapes=[
            pltpu.VMEM((1, HEAD), F32),
            pltpu.VMEM((1, width), F32),
            pltpu.VMEM((1, width), F32),
            pltpu.VMEM((piece, width), BF),
            pltpu.VMEM((count, BLK, d), BF),
            pltpu.VMEM((2, BLK, d), BF),
            pltpu.VMEM((2, BLK, HEAD), F32),
            pltpu.VMEM((2, BLK, HEAD), F32),
            pltpu.VMEM((width, qcols), BF),
            pltpu.VMEM((width, 2 * HEAD), BF),
            pltpu.VMEM((qcols, width), BF),
            pltpu.VMEM((2, BLK, d), BF),
            pltpu.VMEM((2, BLK, d), BF),
            pltpu.VMEM((2, BLK, d), BF),
            pltpu.VMEM((2, BLK, d // 2), BF),
            pltpu.VMEM((2, BLK, d // 2), BF),
            pltpu.VMEM((2, BLK, qcols), F32),
            pltpu.VMEM((2, BLK, 2 * HEAD), F32),
            pltpu.VMEM((2, BLK, HEAD), F32),
            pltpu.VMEM((2, BLK, HEAD), F32),
            pltpu.VMEM((heads * 256, HEAD), BF),
            pltpu.VMEM((8, 8 * BLK, 2 * HEAD), BF),
            pltpu.VMEM((8, heads * 256), F32),
            pltpu.VMEM((HEAD + 16, heads * 256), F32),
            pltpu.VMEM((2, 8 * BLK, 512), F32),
            pltpu.VMEM((2, 8 * BLK, 512), BF),
            pltpu.VMEM((2, 8, 512), F32),
            pltpu.VMEM((256, qcols), BF),
            pltpu.VMEM((4, BLK, d), F32),
            pltpu.VMEM((4, BLK, d), F32),
            pltpu.VMEM((4, piece, d), BF),
            pltpu.VMEM((4, piece, d), BF),
            pltpu.VMEM((4, piece, d), BF),
            pltpu.VMEM((4, piece, d), BF),
            pltpu.VMEM((4, piece, d), BF),
            pltpu.VMEM((4, piece, d), BF),
            pltpu.VMEM((4, piece, d), BF),
            pltpu.SemaphoreType.DMA((nsem,)),
            pltpu.SemaphoreType.DMA((nsem,)),
            pltpu.SemaphoreType.DMA((12,)),
        ],
        compiler_params=pltpu.CompilerParams(
            collective_id=0, has_side_effects=True, vmem_limit_bytes=54 * 1024 * 1024
        ),
    )(
        sel_blocks, freqs, norm_gain.reshape(1, width), router_weight.reshape(1, width),
        resid.reshape(count, BLK, d), w_query, w_key, value_projection, w_out,
    )
    return result


def solution(mesh):
    return jax.shard_map(
        on_device,
        mesh=mesh,
        in_specs=(
            P("ctx", "tp"),
            P("ctx"),
            P(),
            P(),
            P(None, "tp"),
            P(None, "tp"),
            P(None, "tp"),
            P("tp", None),
        ),
        out_specs=P(("ctx", "tp"), None),
        check_vma=False,
    )
```
